32 devices in a mesh: rep: 1 (over z), dp: 32 (over y, x, core).
Axes of the slice: x: 4, y: 4, z: 1, core: 2. Of those that a mesh axis runs over, the one named last changes fastest.
The devices are a block of a 4x4x8 slice.
Arguments:
- audio_x: bfloat16 [32, 1500, 384], P(('rep', 'dp'))
- attn_w: bfloat16 [2, 4, 384, 384], P(None, None, None, 'dp')
- fc1_w: bfloat16 [2, 384, 1536], P(None, None, 'dp')
- fc2_w: bfloat16 [2, 1536, 384], P(None, 'dp')
- vec_d: bfloat16 [2, 8, 384], P(None, None, 'dp')
- b1_vec: bfloat16 [2, 1536], P(None, 'dp')
Outputs:
- output: bfloat16 [32, 1500, 384], P(('rep', 'dp'))
All inputs are finite; a program needn't handle non-finite values.
Results may differ from the reference program's by a relative error of at most 0.0135751.
Values are sent between devices in bfloat16 or wider.
A program may use at most 768 MiB of HBM per device.

```python
import jax
import jax.numpy as jnp
from jax import lax

AUDIOS = 32
FRAMES = 1500
D_MODEL = 384
NUM_HEADS = 6
HEAD_DIM = 64
FF_DIM = 1536
LAYERS = 2
LN_EPSILON = 1e-5


def setup_inputs(seed: int = 0, part: int = 0) -> dict:
    root = jax.random.key(seed)
    key_x, key_attn, key_up, key_down, key_vec, key_bias = jax.random.split(root, 6)
    audio_x = jax.random.normal(jax.random.fold_in(key_x, part), (AUDIOS, FRAMES, D_MODEL), jnp.float32)
    in_scale = D_MODEL ** -0.5
    attn_gain = jnp.array([1.6, 1.6, 1.0, 1.0], jnp.float32).reshape(1, 4, 1, 1)
    attn_w = jax.random.normal(key_attn, (LAYERS, 4, D_MODEL, D_MODEL), jnp.float32) * (attn_gain * in_scale)
    fc1_w = jax.random.normal(key_up, (LAYERS, D_MODEL, FF_DIM), jnp.float32) * in_scale
    fc2_w = jax.random.normal(key_down, (LAYERS, FF_DIM, D_MODEL), jnp.float32) * FF_DIM ** -0.5
    vec_base = jnp.array([0.0, 0.0, 0.0, 0.0, 1.0, 0.0, 1.0, 0.0], jnp.float32).reshape(1, 8, 1)
    vec_spread = jnp.array([0.5, 0.5, 0.3, 0.3, 0.3, 0.3, 0.3, 0.3], jnp.float32).reshape(1, 8, 1)
    vec_d = vec_base + vec_spread * jax.random.normal(key_vec, (LAYERS, 8, D_MODEL), jnp.float32)
    b1_vec = 0.5 * jax.random.normal(key_bias, (LAYERS, FF_DIM), jnp.float32)
    return {'audio_x': audio_x.astype(jnp.bfloat16), 'attn_w': attn_w.astype(jnp.bfloat16), 'fc1_w': fc1_w.astype(jnp.bfloat16), 'fc2_w': fc2_w.astype(jnp.bfloat16), 'vec_d': vec_d.astype(jnp.bfloat16), 'b1_vec': b1_vec.astype(jnp.bfloat16)}


def layer_norm(hidden, gain, shift):
    x_f32 = hidden.astype(jnp.float32)
    mean_val = jnp.mean(x_f32, axis=-1, keepdims=True)
    centered = x_f32 - mean_val
    variance = jnp.mean(centered * centered, axis=-1, keepdims=True)
    scaled = centered * lax.rsqrt(variance + LN_EPSILON)
    return (scaled * gain.astype(jnp.float32) + shift.astype(jnp.float32)).astype(jnp.bfloat16)


def query_block(frames):
    return max([cand_len for cand_len in range(1, 129) if frames % cand_len == 0])


def audio_layer(hidden, w_attn, w_up, w_down, vec_rows, b_up):
    qk_scale = HEAD_DIM ** -0.25
    q_len = query_block(FRAMES)
    normed = layer_norm(hidden, vec_rows[4], vec_rows[5])
    q_proj = ((jnp.dot(normed, w_attn[0], preferred_element_type=jnp.float32) + vec_rows[0].astype(jnp.float32)) * qk_scale).astype(jnp.bfloat16)
    k_proj = (jnp.dot(normed, w_attn[1], preferred_element_type=jnp.float32) * qk_scale).astype(jnp.bfloat16)
    v_proj = (jnp.dot(normed, w_attn[2], preferred_element_type=jnp.float32) + vec_rows[1].astype(jnp.float32)).astype(jnp.bfloat16)
    q_tiles = q_proj.reshape(FRAMES // q_len, q_len, NUM_HEADS, HEAD_DIM).astype(jnp.float32)
    k_heads = k_proj.reshape(FRAMES, NUM_HEADS, HEAD_DIM).astype(jnp.float32)
    v_heads = v_proj.reshape(FRAMES, NUM_HEADS, HEAD_DIM).astype(jnp.float32)

    def one_tile(q_tile):
        scores = jnp.einsum('qhd,khd->hqk', q_tile, k_heads)
        attn_prob = jax.nn.softmax(scores, axis=-1).astype(jnp.bfloat16).astype(jnp.float32)
        return jnp.einsum('hqk,khd->qhd', attn_prob, v_heads).astype(jnp.bfloat16)

    attn_o = lax.map(one_tile, q_tiles).reshape(FRAMES, D_MODEL)
    attn_out = jnp.dot(attn_o, w_attn[3], preferred_element_type=jnp.float32) + vec_rows[2].astype(jnp.float32)
    mid_state = (hidden.astype(jnp.float32) + attn_out).astype(jnp.bfloat16)
    normed_mid = layer_norm(mid_state, vec_rows[6], vec_rows[7])
    up_proj = jnp.dot(normed_mid, w_up, preferred_element_type=jnp.float32) + b_up.astype(jnp.float32)
    gelu_out = jax.nn.gelu(up_proj, approximate=False).astype(jnp.bfloat16)
    down_proj = jnp.dot(gelu_out, w_down, preferred_element_type=jnp.float32) + vec_rows[3].astype(jnp.float32)
    return (mid_state.astype(jnp.float32) + down_proj).astype(jnp.bfloat16)


def reference(audio_x, attn_w, fc1_w, fc2_w, vec_d, b1_vec):
    def layer_step(hidden, params):
        w_attn, w_up, w_down, vec_rows, b_up = params
        layer_out = lax.map(lambda audio_one: audio_layer(audio_one, w_attn, w_up, w_down, vec_rows, b_up), hidden)
        return layer_out, None

    final_x, unused_y = lax.scan(layer_step, audio_x, (attn_w, fc1_w, fc2_w, vec_d, b1_vec))
    return final_x
```

```python
import functools
import math

import jax
import jax.numpy as jnp
from jax import lax
from jax.experimental import pallas as pl
from jax.experimental.pallas import tpu as pltpu
from jax.sharding import PartitionSpec as P

HEAD_DIM = 64
LN_EPSILON = 1e-5
LANES = 128
TILE = 512
F32, BF16 = jnp.float32, jnp.bfloat16
NT = (((1,), (1,)), ((), ()))


def mm(a, b):
    return jnp.dot(a, b, preferred_element_type=F32)


def mm_nt(a, b):
    return lax.dot_general(a, b, NT, preferred_element_type=F32)


def eye(n):
    row = lax.broadcasted_iota(jnp.int32, (n, n), 0)
    col = lax.broadcasted_iota(jnp.int32, (n, n), 1)
    return (row == col).astype(F32).astype(BF16)


def kernel(n, x_ref, w_ref, out_ref, g_ref, wa_ref, w2t_ref, h_ref, a_ref, q_ref, k_ref, v_ref, o_ref, z_ref,
           s0_ref, s1_ref, m0_ref, m1_ref, send_sem, recv_sem, fsend_sem, frecv_sem):
    layers, rows, width = w_ref.shape
    _, frames, model = x_ref.shape
    aug = wa_ref.shape[2]
    heads = model // HEAD_DIM
    pairs = heads // 2
    hidden = z_ref.shape[0]
    tiles = h_ref.shape[0]
    keys = s0_ref.shape[0]
    side = math.isqrt(n // 2)
    chips = n // 2

    me = lax.axis_index("dp")
    core = lax.rem(me, 2)
    chip = me // 2
    partner = me + 1 - 2 * core

    def peer(k, sign):
        dy, dx = divmod(k, side)
        y = lax.rem(chip // side + sign * dy + side, side)
        x = lax.rem(lax.rem(chip, side) + sign * dx + side, side)
        return 2 * (y * side + x) + core

    barrier = pltpu.get_barrier_semaphore()
    for k in range(chips):
        pl.semaphore_signal(barrier, inc=1, device_id={"dp": peer(k, 1) if k else partner})
    pl.semaphore_wait(barrier, chips)

    pieces = []
    for layer in range(layers):
        pieces += [(layer, 0, aug), (layer, aug, width - aug)]

    def slot(ref, piece, dev):
        layer, lo, size = pieces[piece]
        return ref.at[layer, pl.ds(pl.multiple_of(dev * rows, 16), rows), pl.ds(lo, size)]

    def send(piece, k):
        layer, lo, size = pieces[piece]
        return pltpu.make_async_remote_copy(
            src_ref=w_ref.at[layer, :, pl.ds(lo, size)], dst_ref=slot(g_ref, piece, me),
            send_sem=send_sem.at[piece, k], recv_sem=recv_sem.at[piece, k],
            device_id={"dp": peer(k, 1) if k else partner})

    def forward(piece, k):
        src = peer(k, -1)
        return pltpu.make_async_remote_copy(
            src_ref=slot(g_ref, piece, src), dst_ref=slot(g_ref, piece, src),
            send_sem=fsend_sem.at[piece, k - 1], recv_sem=frecv_sem.at[piece, k - 1],
            device_id={"dp": partner})

    def start_forward(piece):
        for k in range(1, chips):
            send(piece, k).wait_recv()
            forward(piece, k).start()

    def wait_piece(piece):
        send(piece, 0).wait_recv()
        for k in range(1, chips):
            forward(piece, k).wait_recv()

    for piece in range(len(pieces)):
        for k in range(chips):
            send(piece, k).start()

    own = pl.ds(pl.multiple_of(me * rows, 16), rows)
    for layer in range(layers):
        g_ref[layer, own, :] = w_ref[layer]
    ones_row = (lax.broadcasted_iota(jnp.int32, (aug - model, TILE), 0) == 0).astype(F32).astype(BF16)
    for t in range(tiles):
        a_ref[t, model:, :] = ones_row
        o_ref[t, model:, :] = ones_row
    zero_half = jnp.zeros((HEAD_DIM, TILE), BF16)
    for h in range(heads):
        other = HEAD_DIM * (1 - h % 2)
        for t in range(tiles):
            q_ref[h, t, other:other + HEAD_DIM, :] = zero_half
        extra = v_ref.shape[1] - HEAD_DIM
        v_ref[h, HEAD_DIM:, :] = (lax.broadcasted_iota(jnp.int32, (extra, v_ref.shape[2]), 0) == 0).astype(F32).astype(BF16)
    eye_m = eye(model)
    h_ref[tiles - 1, :, :] = jnp.zeros((model, TILE), BF16)
    for t in range(tiles):
        size = min(TILE, frames - t * TILE)
        h_ref[t, :, 0:size] = mm_nt(eye_m, x_ref[0, t * TILE:t * TILE + size, :]).astype(BF16)

    def layer_norm(z, gain, shift):
        mean = jnp.sum(z, axis=0, keepdims=True) * (1.0 / model)
        c = z - mean
        var = jnp.sum(c * c, axis=0, keepdims=True) * (1.0 / model)
        return (c * lax.rsqrt(var + LN_EPSILON) * gain + shift).astype(BF16)

    def column(j, lane):
        return wa_ref[j, :, lane:lane + 1].astype(F32)

    def unpack(layer):
        block = 4 * HEAD_DIM
        row = lax.broadcasted_iota(jnp.int32, (block, block), 0)
        col = lax.broadcasted_iota(jnp.int32, (block, block), 1)
        perm = (col == lax.rem(row, HEAD_DIM) * 4 + row // HEAD_DIM).astype(F32).astype(BF16)
        for h in range(heads):
            mixed = mm(perm, g_ref[layer, h * block:(h + 1) * block, 0:aug]).astype(BF16)
            for j in range(4):
                wa_ref[j, h * HEAD_DIM:(h + 1) * HEAD_DIM, :] = mixed[j * HEAD_DIM:(j + 1) * HEAD_DIM]

    scale = HEAD_DIM ** -0.25
    eye_k = eye(TILE // 2)

    def pre(t):
        lanes = pl.ds(pl.multiple_of(t * TILE, TILE), TILE)
        a_ref[t, 0:model, :] = layer_norm(h_ref[t].astype(F32), column(0, model + 1), column(1, model + 1))
        a = a_ref[t]
        q = (mm(wa_ref[0], a) * scale).astype(BF16)
        for h in range(heads):
            half = HEAD_DIM * (h % 2)
            q_ref[h, t, half:half + HEAD_DIM, :] = q[h * HEAD_DIM:(h + 1) * HEAD_DIM]
        kt = (mm(wa_ref[1], a) * scale).astype(BF16)
        half = TILE // 2
        for b in range(2):
            kn = mm_nt(eye_k, kt[:, b * half:(b + 1) * half]).astype(BF16)
            for p in range(pairs):
                k_ref[p, pl.ds(pl.multiple_of(t * TILE + b * half, half), half), :] = kn[:, p * LANES:(p + 1) * LANES]
        v = mm(wa_ref[2], a).astype(BF16)
        for h in range(heads):
            v_ref[h, 0:HEAD_DIM, lanes] = v[h * HEAD_DIM:(h + 1) * HEAD_DIM]

    s_refs, m_refs = (s0_ref, s1_ref), (m0_ref, m1_ref)

    def scores(p, hh, t, buf):
        s = mm(k_ref[p, 0:keys, :], q_ref[2 * p + hh, t])
        last = keys - 8
        row = lax.broadcasted_iota(jnp.int32, (8, TILE), 0) + last
        tail = jnp.where(row < frames, s[last:], -jnp.inf)
        s_refs[buf][0:last, :] = s[0:last]
        s_refs[buf][last:, :] = tail
        m_refs[buf][...] = jnp.maximum(jnp.max(s[0:last], axis=0, keepdims=True), jnp.max(tail, axis=0, keepdims=True))

    def values(p, hh, t, buf):
        h = 2 * p + hh
        e = jnp.exp(s_refs[buf][...] - m_refs[buf][...]).astype(BF16)
        o = mm(v_ref[h, :, 0:keys], e)
        inv = 1.0 / o[HEAD_DIM:HEAD_DIM + 1]
        o_ref[t, pl.ds(pl.multiple_of(h * HEAD_DIM, HEAD_DIM), HEAD_DIM), :] = (o[0:HEAD_DIM] * inv).astype(BF16)

    def attention(events):
        steps = [(hh, t) for hh in range(2) for t in range(tiles)]

        def body(p, carry):
            for at, event in events.items():
                pl.when(p == at)(event)
            for j, (hh, t) in enumerate(steps):
                scores(p, hh, t, j % 2)
                if j:
                    values(p, *steps[j - 1], (j - 1) % 2)
                else:
                    values(jnp.maximum(p - 1, 0), *steps[-1], 1)
            return carry

        lax.fori_loop(0, pairs, body, 0)
        values(pairs - 1, *steps[-1], 1)

    def unpack_mlp(layer):
        for b in range(hidden // TILE):
            w2 = g_ref[layer, b * TILE:(b + 1) * TILE, 2 * aug:2 * aug + model]
            w2t_ref[:, b * TILE:(b + 1) * TILE] = mm_nt(eye_m, w2).astype(BF16)

    def post(layer, t):
        r = h_ref[t].astype(F32) + mm(wa_ref[3], o_ref[t])
        r = r.astype(BF16)
        a_ref[t, 0:model, :] = layer_norm(r.astype(F32), column(2, model + 1), column(3, model + 1))
        c = a_ref[t]
        step = 2 * LANES
        for b in range(hidden // step):
            u = mm(g_ref[layer, b * step:(b + 1) * step, aug:2 * aug], c)
            z_ref[b * step:(b + 1) * step, :] = (0.5 * u * (1.0 + lax.erf(u * (2.0 ** -0.5)))).astype(BF16)
        y = r.astype(F32) + (mm(w2t_ref[...], z_ref[...]) + column(0, model + 2))
        h_ref[t] = y.astype(BF16)

    for layer in range(layers):
        piece = 2 * layer
        if layer == 0:
            start_forward(piece)
        wait_piece(piece)
        unpack(layer)
        lax.fori_loop(0, tiles, lambda t, c: (pre(t), c)[1], 0)
        attention({pairs - 1: functools.partial(start_forward, piece + 1)})
        if layer + 1 < layers:
            start_forward(piece + 2)
        wait_piece(piece + 1)
        unpack_mlp(layer)
        lax.fori_loop(0, tiles, lambda t, c, layer=layer: (post(layer, t), c)[1], 0)

    for t in range(tiles):
        for b in range(2):
            lo = t * TILE + b * (TILE // 2)
            size = min(TILE // 2, frames - lo)
            y = mm_nt(eye_k, h_ref[t, :, b * (TILE // 2):(b + 1) * (TILE // 2)]).astype(BF16)
            out_ref[0, lo:lo + size, :] = y[0:size]

    for piece in range(len(pieces)):
        for k in range(chips):
            send(piece, k).wait_send()
        for k in range(1, chips):
            forward(piece, k).wait_send()


def solution(mesh):
    n = mesh.shape["dp"]

    def body(audio_x, attn_w, fc1_w, fc2_w, vec_d, b1_vec):
        layers, four, model, cols = attn_w.shape
        hidden_cols = fc1_w.shape[2]
        batch, frames, _ = audio_x.shape
        hidden = hidden_cols * n
        aug = model + LANES
        rows = four * cols
        vec = jnp.moveaxis(vec_d, 1, 2)
        bias = jnp.stack([vec[..., 0], jnp.zeros_like(vec[..., 0]), vec[..., 1], vec[..., 2]], -1)
        b2 = jnp.pad(vec[..., 3:4], ((0, 0), (0, 0), (0, four - 1)))
        extra = jnp.stack([bias, vec[..., 4:8], b2], -1)
        extra = jnp.pad(extra, ((0, 0), (0, 0), (0, 0), (0, LANES - extra.shape[-1])))
        attn = jnp.concatenate([jnp.transpose(attn_w, (0, 3, 1, 2)), extra], -1).reshape(layers, rows, aug)
        b1 = jnp.pad(b1_vec[..., None], ((0, 0), (0, 0), (0, LANES - 1)))
        packed = jnp.concatenate([attn, jnp.transpose(fc1_w, (0, 2, 1)), b1, fc2_w], -1)

        tiles = -(-frames // TILE)
        padded = tiles * TILE
        keys = -(-frames // 16) * 16
        heads = model // HEAD_DIM
        chips = n // 2
        pieces = 2 * layers
        vmem = pl.BlockSpec(memory_space=pltpu.VMEM)
        return pl.pallas_call(
            functools.partial(kernel, n),
            out_shape=jax.ShapeDtypeStruct(audio_x.shape, audio_x.dtype),
            in_specs=[vmem, vmem],
            out_specs=vmem,
            scratch_shapes=[
                pltpu.VMEM((layers, n * rows, packed.shape[-1]), BF16),
                pltpu.VMEM((four, model, aug), BF16),
                pltpu.VMEM((model, hidden), BF16),
                pltpu.VMEM((tiles, model, TILE), BF16),
                pltpu.VMEM((tiles, aug, TILE), BF16),
                pltpu.VMEM((heads, tiles, LANES, TILE), BF16),
                pltpu.VMEM((heads // 2, padded, LANES), BF16),
                pltpu.VMEM((heads, HEAD_DIM + 16, padded), BF16),
                pltpu.VMEM((tiles, aug, TILE), BF16),
                pltpu.VMEM((hidden, TILE), BF16),
                pltpu.VMEM((keys, TILE), F32),
                pltpu.VMEM((keys, TILE), F32),
                pltpu.VMEM((1, TILE), F32),
                pltpu.VMEM((1, TILE), F32),
                pltpu.SemaphoreType.DMA((pieces, chips)),
                pltpu.SemaphoreType.DMA((pieces, chips)),
                pltpu.SemaphoreType.DMA((pieces, chips - 1)),
                pltpu.SemaphoreType.DMA((pieces, chips - 1)),
            ],
            compiler_params=pltpu.CompilerParams(
                collective_id=0, has_side_effects=True, vmem_limit_bytes=60 * 1024 * 1024),
        )(audio_x, packed)

    return jax.shard_map(
        body, mesh=mesh,
        in_specs=(P(('rep', 'dp')), P(None, None, None, 'dp'), P(None, None, 'dp'), P(None, 'dp', None), P(None, None, 'dp'), P(None, 'dp')),
        out_specs=P(('rep', 'dp')), check_vma=False)
```

```python
import functools

import jax
import jax.numpy as jnp
from jax import lax
from jax.experimental import pallas as pl
from jax.experimental.pallas import tpu as pltpu
from jax.sharding import PartitionSpec as P

HEAD_DIM = 64
LN_EPSILON = 1e-5
LANES = 128
TILE = 512
F32, BF16 = jnp.float32, jnp.bfloat16
NT = (((1,), (1,)), ((), ()))


def mm(a, b):
    return jnp.dot(a, b, preferred_element_type=F32)


def mm_nt(a, b):
    return lax.dot_general(a, b, NT, preferred_element_type=F32)


def eye(n):
    row = lax.broadcasted_iota(jnp.int32, (n, n), 0)
    col = lax.broadcasted_iota(jnp.int32, (n, n), 1)
    return (row == col).astype(F32).astype(BF16)


RING = 4


def relay_plan():
    messages, complete = [], {}

    def add(*message):
        messages.append(message)
        return len(messages) - 1

    for half in range(2):
        d1, d2 = half, 1 - half

        def at(a, b):
            offset = [0, 0]
            offset[d1], offset[d2] = a % RING, b % RING
            return tuple(offset)

        both = (1, -1)
        part = {1: 0, -1: 1}
        own = {(d, s): add(1, half, None, at(0, 0), d, s, ()) for d in (d1, d2) for s in both}
        far = {s: add(2, half, part[s], at(-s, 0), d1, s, (own[d1, s],)) for s in both}
        side = {(s, r): add(2, half, None, at(-s, 0), d2, r, (own[d1, s],)) for s in both for r in both}
        col = {r: add(2, half, part[r], at(0, -r), d2, r, (own[d2, r],)) for r in both}
        turn = {r: add(3, half, None, at(2, 0), d2, r, (far[1], far[-1])) for r in both}
        diag = {(s, r): add(3, half, part[r], at(-s, -r), d2, r, (side[s, r],)) for s in both for r in both}
        last = {r: add(4, half, part[r], at(2, -r), d2, r, (turn[r],)) for r in both}
        for s in both:
            complete[half, at(-s, 0)] = (own[d1, s],)
            complete[half, at(0, -s)] = (own[d2, s],)
            complete[half, at(2, -s)] = (turn[s],)
            complete[half, at(-s, 2)] = (diag[s, 1], diag[s, -1])
            for r in both:
                complete[half, at(-s, -r)] = (side[s, r],)
        complete[half, at(2, 0)] = (far[1], far[-1])
        complete[half, at(0, 2)] = (col[1], col[-1])
        complete[half, at(2, 2)] = (last[1], last[-1])
    return messages, complete


MESSAGES, COMPLETE = relay_plan()
BLOCKS = list(COMPLETE)


class Planner:
    def __init__(self):
        self.arrived, self.passed = set(), set()

    def step(self, piece, step):
        actions = []
        for m, message in enumerate(MESSAGES):
            if message[0] == step:
                actions += self.need(piece, message[-1])
                actions.append(("start", piece, m))
        if step == 1:
            actions.append(("pass", piece, len(BLOCKS)))
        return actions + self.hand_over(piece)

    def need(self, piece, deps):
        actions = [("wait", piece, m) for m in deps if (piece, m) not in self.arrived]
        self.arrived.update((piece, m) for m in deps)
        return actions

    def hand_over(self, piece, everything=False):
        actions = []
        for b, block in enumerate(BLOCKS):
            if (piece, b) in self.passed:
                continue
            if everything:
                actions += self.need(piece, COMPLETE[block])
            if all((piece, m) in self.arrived for m in COMPLETE[block]):
                actions.append(("pass", piece, b))
                self.passed.add((piece, b))
        if everything:
            actions += self.need(piece, range(len(MESSAGES)))
        return actions


def kernel(n, x_hbm, attn_ref, fc1_ref, fc2_ref, vec_ref, b1_ref, out_ref, w_ref, g_ref, wa_ref, w2t_ref, x_ref, h_ref, a_ref,
           q_ref, k_ref, v_ref, o_ref, z_ref, s0_ref, s1_ref, m0_ref, m1_ref, x_sem, send_sem, recv_sem, fsend_sem, frecv_sem):
    layers, rows, width = w_ref.shape
    frames, model = x_ref.shape
    aug = wa_ref.shape[2]
    heads = model // HEAD_DIM
    pairs = heads // 2
    hidden = z_ref.shape[0]
    tiles = h_ref.shape[0]
    keys = s0_ref.shape[0]

    fetch_x = pltpu.make_async_copy(x_hbm.at[0], x_ref, x_sem)
    fetch_x.start()

    me = lax.axis_index("dp")
    core = lax.rem(me, 2)
    chip = me // 2
    chip_x, chip_y = lax.rem(chip, RING), chip // RING

    def device(offset):
        x = lax.rem(chip_x + offset[0] + RING, RING)
        y = lax.rem(chip_y + offset[1] + RING, RING)
        return 2 * (y * RING + x) + core

    partner = me + 1 - 2 * core
    neighbour = {(d, s): device((s, 0) if d == 0 else (0, s)) for d in range(2) for s in (1, -1)}

    barrier = pltpu.get_barrier_semaphore()
    for dev in [*neighbour.values(), partner]:
        pl.semaphore_signal(barrier, inc=1, device_id={"dp": dev})

    def pick(layer, want):
        row = lax.broadcasted_iota(jnp.int32, (rows, vec_ref.shape[1]), 0)
        col = lax.broadcasted_iota(jnp.int32, (rows, vec_ref.shape[1]), 1)
        sel = jnp.zeros(row.shape, F32)
        for j, r in enumerate(want):
            if r is not None:
                sel = jnp.where((lax.rem(row, 4) == j) & (col == r), 1.0, sel)
        spread = mm(sel, vec_ref[layer].astype(F32))
        row = lax.broadcasted_iota(jnp.int32, spread.shape, 0)
        col = lax.broadcasted_iota(jnp.int32, spread.shape, 1)
        return jnp.sum(jnp.where(row // 4 == col, spread, 0.0), axis=1, keepdims=True)

    lane = lax.broadcasted_iota(jnp.int32, (rows, LANES), 1)
    for layer in range(layers):
        w_ref[layer, :, 0:model] = attn_ref[layer]
        entry = [pick(layer, want) for want in ((0, None, 1, 2), (4, 5, 6, 7), (3, None, None, None))]
        extra = jnp.where(lane == 0, entry[0], jnp.where(lane == 1, entry[1], jnp.where(lane == 2, entry[2], 0.0)))
        w_ref[layer, :, model:aug] = extra.astype(BF16)
        w_ref[layer, :, aug:aug + model] = fc1_ref[layer]
        row = lax.broadcasted_iota(jnp.int32, (rows, rows), 0)
        col = lax.broadcasted_iota(jnp.int32, (rows, rows), 1)
        b1 = jnp.sum(jnp.where(row == col, b1_ref[layer:layer + 1, :].astype(F32), 0.0), axis=1, keepdims=True)
        w_ref[layer, :, aug + model:2 * aug] = jnp.where(lane == 0, b1, 0.0).astype(BF16)
        w_ref[layer, :, 2 * aug:width] = fc2_ref[layer]

    own = pl.ds(pl.multiple_of(me * rows, 16), rows)
    for layer in range(layers):
        g_ref[layer, own, :] = w_ref[layer]
    ones_row = (lax.broadcasted_iota(jnp.int32, (aug - model, TILE), 0) == 0).astype(F32).astype(BF16)
    for t in range(tiles):
        a_ref[t, model:, :] = ones_row
        o_ref[t, model:, :] = ones_row

    pl.semaphore_wait(barrier, len(neighbour) + 1)

    pieces = [(0, 0, aug), (0, aug, width - aug)] + [(layer, 0, width) for layer in range(1, layers)]

    def lanes_of(piece, half, quarter):
        _, lo, size = pieces[piece]
        units = size // LANES
        first = -(-units // 2)
        lo, units = (lo, first) if half == 0 else (lo + first * LANES, units - first)
        first = -(-units // 2)
        if quarter is not None:
            lo, units = (lo, first) if quarter == 0 else (lo + first * LANES, units - first)
        return pl.ds(lo, units * LANES)

    def slot(piece, dev, lanes):
        return g_ref.at[pieces[piece][0], pl.ds(pl.multiple_of(dev * rows, 16), rows), lanes]

    def relay(piece, m):
        step, half, quarter, offset, d, s, _ = MESSAGES[m]
        lanes = lanes_of(piece, half, quarter)
        dst = slot(piece, device(offset), lanes)
        src = w_ref.at[pieces[piece][0], :, lanes] if step == 1 else dst
        return pltpu.make_async_remote_copy(
            src_ref=src, dst_ref=dst, send_sem=send_sem.at[piece, m], recv_sem=recv_sem.at[piece, m],
            device_id={"dp": neighbour[d, s]})

    def hand(piece, b):
        if b == len(BLOCKS):
            lanes = pl.ds(*pieces[piece][1:])
            src, dst = w_ref.at[pieces[piece][0], :, lanes], slot(piece, me, lanes)
        else:
            half, offset = BLOCKS[b]
            src = dst = slot(piece, device(offset), lanes_of(piece, half, None))
        return pltpu.make_async_remote_copy(
            src_ref=src, dst_ref=dst, send_sem=fsend_sem.at[piece, b], recv_sem=frecv_sem.at[piece, b],
            device_id={"dp": partner})

    def run(actions):
        for kind, piece, index in actions:
            if kind == "start":
                relay(piece, index).start()
            elif kind == "wait":
                relay(piece, index).wait_recv()
            else:
                hand(piece, index).start()

    def finish(piece):
        run(plan.hand_over(piece, everything=True))
        for b in range(len(BLOCKS) + 1):
            hand(piece, b).wait_recv()

    plan = Planner()
    run(plan.step(0, 1))

    zero_half = jnp.zeros((HEAD_DIM, TILE), BF16)
    for h in range(heads):
        other = HEAD_DIM * (1 - h % 2)
        for t in range(tiles):
            q_ref[h, t, other:other + HEAD_DIM, :] = zero_half
        extra = v_ref.shape[1] - HEAD_DIM
        v_ref[h, HEAD_DIM:, :] = (lax.broadcasted_iota(jnp.int32, (extra, v_ref.shape[2]), 0) == 0).astype(F32).astype(BF16)

    run(plan.step(0, 2))

    eye_m = eye(model)
    h_ref[tiles - 1, :, :] = jnp.zeros((model, TILE), BF16)
    fetch_x.wait()
    for t in range(tiles):
        size = min(TILE, frames - t * TILE)
        h_ref[t, :, 0:size] = mm_nt(eye_m, x_ref[t * TILE:t * TILE + size, :]).astype(BF16)

    run(plan.step(0, 3))
    run(plan.step(0, 4))
    run(plan.step(1, 1))

    def layer_norm(z, gain, shift):
        mean = jnp.sum(z, axis=0, keepdims=True) * (1.0 / model)
        c = z - mean
        var = jnp.sum(c * c, axis=0, keepdims=True) * (1.0 / model)
        return (c * lax.rsqrt(var + LN_EPSILON) * gain + shift).astype(BF16)

    def column(j, lane):
        return wa_ref[j, :, lane:lane + 1].astype(F32)

    def unpack(layer):
        block = 4 * HEAD_DIM
        row = lax.broadcasted_iota(jnp.int32, (block, block), 0)
        col = lax.broadcasted_iota(jnp.int32, (block, block), 1)
        perm = (col == lax.rem(row, HEAD_DIM) * 4 + row // HEAD_DIM).astype(F32).astype(BF16)
        for h in range(heads):
            mixed = mm(perm, g_ref[layer, h * block:(h + 1) * block, 0:aug]).astype(BF16)
            for j in range(4):
                wa_ref[j, h * HEAD_DIM:(h + 1) * HEAD_DIM, :] = mixed[j * HEAD_DIM:(j + 1) * HEAD_DIM]

    scale = HEAD_DIM ** -0.25
    eye_k = eye(TILE // 2)

    def pre(t):
        lanes = pl.ds(pl.multiple_of(t * TILE, TILE), TILE)
        a_ref[t, 0:model, :] = layer_norm(h_ref[t].astype(F32), column(0, model + 1), column(1, model + 1))
        a = a_ref[t]
        q = (mm(wa_ref[0], a) * scale).astype(BF16)
        for h in range(heads):
            half = HEAD_DIM * (h % 2)
            q_ref[h, t, half:half + HEAD_DIM, :] = q[h * HEAD_DIM:(h + 1) * HEAD_DIM]
        kt = (mm(wa_ref[1], a) * scale).astype(BF16)
        half = TILE // 2
        for b in range(2):
            kn = mm_nt(eye_k, kt[:, b * half:(b + 1) * half]).astype(BF16)
            for p in range(pairs):
                k_ref[p, pl.ds(pl.multiple_of(t * TILE + b * half, half), half), :] = kn[:, p * LANES:(p + 1) * LANES]
        v = mm(wa_ref[2], a).astype(BF16)
        for h in range(heads):
            v_ref[h, 0:HEAD_DIM, lanes] = v[h * HEAD_DIM:(h + 1) * HEAD_DIM]

    s_refs, m_refs = (s0_ref, s1_ref), (m0_ref, m1_ref)

    def scores(p, hh, t, buf):
        s = mm(k_ref[p, 0:keys, :], q_ref[2 * p + hh, t])
        last = keys - 8
        row = lax.broadcasted_iota(jnp.int32, (8, TILE), 0) + last
        tail = jnp.where(row < frames, s[last:], -jnp.inf)
        s_refs[buf][0:last, :] = s[0:last]
        s_refs[buf][last:, :] = tail
        m_refs[buf][...] = jnp.maximum(jnp.max(s[0:last], axis=0, keepdims=True), jnp.max(tail, axis=0, keepdims=True))

    def values(p, hh, t, buf):
        h = 2 * p + hh
        e = jnp.exp(s_refs[buf][...] - m_refs[buf][...]).astype(BF16)
        o = mm(v_ref[h, :, 0:keys], e)
        inv = 1.0 / o[HEAD_DIM:HEAD_DIM + 1]
        o_ref[t, pl.ds(pl.multiple_of(h * HEAD_DIM, HEAD_DIM), HEAD_DIM), :] = (o[0:HEAD_DIM] * inv).astype(BF16)

    def attention(events):
        steps = [(hh, t) for hh in range(2) for t in range(tiles)]

        def body(p, carry):
            for j, (hh, t) in enumerate(steps):
                for (at, when), actions in events.items():
                    if when == j:
                        pl.when(p == at)(functools.partial(run, actions))
                scores(p, hh, t, j % 2)
                if j:
                    values(p, *steps[j - 1], (j - 1) % 2)
                else:
                    values(jnp.maximum(p - 1, 0), *steps[-1], 1)
            return carry

        lax.fori_loop(0, pairs, body, 0)
        values(pairs - 1, *steps[-1], 1)

    def unpack_mlp(layer):
        for b in range(hidden // TILE):
            w2 = g_ref[layer, b * TILE:(b + 1) * TILE, 2 * aug:2 * aug + model]
            w2t_ref[:, b * TILE:(b + 1) * TILE] = mm_nt(eye_m, w2).astype(BF16)

    def post(layer, t):
        r = h_ref[t].astype(F32) + mm(wa_ref[3], o_ref[t])
        r = r.astype(BF16)
        a_ref[t, 0:model, :] = layer_norm(r.astype(F32), column(2, model + 1), column(3, model + 1))
        c = a_ref[t]
        step = 2 * LANES
        for b in range(hidden // step):
            u = mm(g_ref[layer, b * step:(b + 1) * step, aug:2 * aug], c)
            z_ref[b * step:(b + 1) * step, :] = (0.5 * u * (1.0 + lax.erf(u * (2.0 ** -0.5)))).astype(BF16)
        y = r.astype(F32) + (mm(w2t_ref[...], z_ref[...]) + column(0, model + 2))
        h_ref[t] = y.astype(BF16)

    for layer in range(layers):
        more = layer + 1 < layers
        if layer == 0:
            finish(0)
        unpack(layer)
        lax.fori_loop(0, tiles, lambda t, c: (pre(t), c)[1], 0)
        events = {}
        if layer == 0:
            run(plan.step(1, 2))
            events[0, 3] = plan.step(1, 3)
            events[1, 0] = plan.step(1, 4)
        if more:
            events.setdefault((1, 0), []).extend(plan.step(layer + 2, 1))
            events[1, 3] = plan.step(layer + 2, 2)
            events[2, 0] = (plan.hand_over(1, everything=True) if layer == 0 else []) + plan.step(layer + 2, 3)
            events[2, 3] = plan.step(layer + 2, 4)
        attention(events)
        if layer == 0:
            finish(1)
        unpack_mlp(layer)
        late = plan.hand_over(layer + 2, everything=True) if more else []

        def tile(t, carry, layer=layer, late=late):
            if late:
                pl.when(t == 1)(functools.partial(run, late))
            post(layer, t)
            return carry

        lax.fori_loop(0, tiles, tile, 0)
        if more:
            finish(layer + 2)

    for t in range(tiles):
        for b in range(2):
            lo = t * TILE + b * (TILE // 2)
            size = min(TILE // 2, frames - lo)
            y = mm_nt(eye_k, h_ref[t, :, b * (TILE // 2):(b + 1) * (TILE // 2)]).astype(BF16)
            out_ref[0, lo:lo + size, :] = y[0:size]

    for piece in range(len(pieces)):
        for m in range(len(MESSAGES)):
            relay(piece, m).wait_send()
        for b in range(len(BLOCKS) + 1):
            hand(piece, b).wait_send()


def solution(mesh):
    n = mesh.shape["dp"]

    def body(audio_x, attn_w, fc1_w, fc2_w, vec_d, b1_vec):
        layers, four, model, cols = attn_w.shape
        hidden_cols = fc1_w.shape[2]
        batch, frames, _ = audio_x.shape
        hidden = hidden_cols * n
        aug = model + LANES
        rows = four * cols
        attn = jnp.transpose(attn_w, (0, 3, 1, 2)).reshape(layers, rows, model)
        fc1 = jnp.transpose(fc1_w, (0, 2, 1))

        tiles = -(-frames // TILE)
        padded = tiles * TILE
        keys = -(-frames // 16) * 16
        heads = model // HEAD_DIM
        pieces = layers + 1
        vmem = pl.BlockSpec(memory_space=pltpu.VMEM)
        return pl.pallas_call(
            functools.partial(kernel, n),
            out_shape=jax.ShapeDtypeStruct(audio_x.shape, audio_x.dtype),
            in_specs=[pl.BlockSpec(memory_space=pl.ANY)] + [vmem] * 5,
            out_specs=vmem,
            scratch_shapes=[
                pltpu.VMEM((layers, rows, 2 * aug + model), BF16),
                pltpu.VMEM((layers, n * rows, 2 * aug + model), BF16),
                pltpu.VMEM((four, model, aug), BF16),
                pltpu.VMEM((model, hidden), BF16),
                pltpu.VMEM((frames, model), BF16),
                pltpu.VMEM((tiles, model, TILE), BF16),
                pltpu.VMEM((tiles, aug, TILE), BF16),
                pltpu.VMEM((heads, tiles, LANES, TILE), BF16),
                pltpu.VMEM((heads // 2, padded, LANES), BF16),
                pltpu.VMEM((heads, HEAD_DIM + 16, padded), BF16),
                pltpu.VMEM((tiles, aug, TILE), BF16),
                pltpu.VMEM((hidden, TILE), BF16),
                pltpu.VMEM((keys, TILE), F32),
                pltpu.VMEM((keys, TILE), F32),
                pltpu.VMEM((1, TILE), F32),
                pltpu.VMEM((1, TILE), F32),
                pltpu.SemaphoreType.DMA,
                pltpu.SemaphoreType.DMA((pieces, len(MESSAGES))),
                pltpu.SemaphoreType.DMA((pieces, len(MESSAGES))),
                pltpu.SemaphoreType.DMA((pieces, len(BLOCKS) + 1)),
                pltpu.SemaphoreType.DMA((pieces, len(BLOCKS) + 1)),
            ],
            compiler_params=pltpu.CompilerParams(
                collective_id=0, has_side_effects=True, vmem_limit_bytes=60 * 1024 * 1024),
        )(audio_x, attn, fc1, fc2_w, vec_d, b1_vec)

    return jax.shard_map(
        body, mesh=mesh,
        in_specs=(P(('rep', 'dp')), P(None, None, None, 'dp'), P(None, None, 'dp'), P(None, 'dp', None), P(None, None, 'dp'), P(None, 'dp')),
        out_specs=P(('rep', 'dp')), check_vma=False)
```

```python
import functools

import jax
import jax.numpy as jnp
from jax import lax
from jax.experimental import pallas as pl
from jax.experimental.pallas import tpu as pltpu
from jax.sharding import PartitionSpec as P

HEAD_DIM = 64
LN_EPSILON = 1e-5
LANES = 128
TILE = 512
F32, BF16 = jnp.float32, jnp.bfloat16
NT = (((1,), (1,)), ((), ()))


def mm(a, b):
    return jnp.dot(a, b, preferred_element_type=F32)


def mm_nt(a, b):
    return lax.dot_general(a, b, NT, preferred_element_type=F32)


def eye(n):
    row = lax.broadcasted_iota(jnp.int32, (n, n), 0)
    col = lax.broadcasted_iota(jnp.int32, (n, n), 1)
    return (row == col).astype(F32).astype(BF16)


RING = 4


def relay_plan():
    messages, complete = [], {}

    def add(*message):
        messages.append(message)
        return len(messages) - 1

    def at(a, b):
        return a % RING, b % RING

    both = (1, -1)
    axes = [(1, 0), (-1, 0), (0, 1), (0, -1)]
    corners = [(a, b) for a in both for b in both]
    own = {to: add(1, (0, 1), at(0, 0), to, ()) for to in axes + corners}
    for (a, b), m in own.items():
        complete[at(-a, -b)] = (m,)
    for part, s in enumerate(both):
        for r in (0, 1, -1):
            m = add(2, (part, 2), at(-s, -r), (s, 0), (own[s, r],))
            complete[at(2, -r)] = complete.get(at(2, -r), ()) + (m,)
            m = add(2, (part, 2), at(-r, -s), (0, s), (own[r, s],))
            complete[at(-r, 2)] = complete.get(at(-r, 2), ()) + (m,)
    for part, (a, b) in enumerate(corners):
        m = add(2, (part, 4), at(-a, -b), (a, b), (own[a, b],))
        complete[at(2, 2)] = complete.get(at(2, 2), ()) + (m,)
    return messages, complete


MESSAGES, COMPLETE = relay_plan()
BLOCKS = list(COMPLETE)


class Planner:
    def __init__(self):
        self.arrived, self.passed = set(), set()

    def step(self, piece, step):
        actions = []
        for m, message in enumerate(MESSAGES):
            if message[0] == step:
                actions += self.need(piece, message[-1])
                actions.append(("start", piece, m))
        if step == 1:
            actions.append(("pass", piece, len(BLOCKS)))
        return actions + self.hand_over(piece)

    def need(self, piece, deps):
        actions = [("wait", piece, m) for m in deps if (piece, m) not in self.arrived]
        self.arrived.update((piece, m) for m in deps)
        return actions

    def hand_over(self, piece, everything=False):
        actions = []
        for b, block in enumerate(BLOCKS):
            if (piece, b) in self.passed:
                continue
            if everything:
                actions += self.need(piece, COMPLETE[block])
            if all((piece, m) in self.arrived for m in COMPLETE[block]):
                actions.append(("pass", piece, b))
                self.passed.add((piece, b))
        if everything:
            actions += self.need(piece, range(len(MESSAGES)))
        return actions


def kernel(n, x_hbm, attn_ref, fc1_ref, fc2_ref, vec_ref, b1_ref, out_hbm, w_ref, row_ref, g_ref, wa_ref, w2t_ref, x_ref, y_ref, h_ref, a_ref,
           q_ref, k_ref, v_ref, o_ref, z_ref, s0_ref, s1_ref, m0_ref, m1_ref, x_sem, out_sem, send_sem, recv_sem, fsend_sem, frecv_sem):
    layers, rows, width = w_ref.shape
    _, frames, model = x_hbm.shape
    aug = wa_ref.shape[2]
    heads = model // HEAD_DIM
    pairs = heads // 2
    hidden = z_ref.shape[0]
    tiles = h_ref.shape[0]
    keys = s0_ref.shape[0]

    fetch_x = pltpu.make_async_copy(x_hbm.at[0], x_ref, x_sem)
    fetch_x.start()

    me = lax.axis_index("dp")
    core = lax.rem(me, 2)
    chip = me // 2
    chip_x, chip_y = lax.rem(chip, RING), chip // RING

    def device(offset):
        x = lax.rem(chip_x + offset[0] + RING, RING)
        y = lax.rem(chip_y + offset[1] + RING, RING)
        return 2 * (y * RING + x) + core

    partner = me + 1 - 2 * core
    neighbour = {to: device(to) for step, _, _, to, _ in MESSAGES if step == 1}

    barrier = pltpu.get_barrier_semaphore()
    for dev in [*neighbour.values(), partner]:
        pl.semaphore_signal(barrier, inc=1, device_id={"dp": dev})

    def pick(layer, want):
        row = lax.broadcasted_iota(jnp.int32, (rows, vec_ref.shape[1]), 0)
        col = lax.broadcasted_iota(jnp.int32, (rows, vec_ref.shape[1]), 1)
        sel = jnp.zeros(row.shape, F32)
        for j, r in enumerate(want):
            if r is not None:
                sel = jnp.where((lax.rem(row, 4) == j) & (col == r), 1.0, sel)
        spread = mm(sel, vec_ref[layer].astype(F32))
        row = lax.broadcasted_iota(jnp.int32, spread.shape, 0)
        col = lax.broadcasted_iota(jnp.int32, spread.shape, 1)
        return jnp.sum(jnp.where(row // 4 == col, spread, 0.0), axis=1, keepdims=True)

    lane = lax.broadcasted_iota(jnp.int32, (rows, LANES), 1)
    for layer in range(layers):
        for c in range(rows // 4):
            row_ref[4 * c:4 * c + 4, :] = attn_ref[layer, c].astype(F32)
        w_ref[layer, :, 0:model] = row_ref[...].astype(BF16)
        entry = [pick(layer, want) for want in ((0, None, 1, 2), (4, 5, 6, 7), (3, None, None, None))]
        extra = jnp.where(lane == 0, entry[0], jnp.where(lane == 1, entry[1], jnp.where(lane == 2, entry[2], 0.0)))
        w_ref[layer, :, model:aug] = extra.astype(BF16)
        w_ref[layer, :, aug:aug + model] = fc1_ref[layer]
        row = lax.broadcasted_iota(jnp.int32, (rows, rows), 0)
        col = lax.broadcasted_iota(jnp.int32, (rows, rows), 1)
        b1 = jnp.sum(jnp.where(row == col, b1_ref[layer:layer + 1, :].astype(F32), 0.0), axis=1, keepdims=True)
        w_ref[layer, :, aug + model:2 * aug] = jnp.where(lane == 0, b1, 0.0).astype(BF16)
        w_ref[layer, :, 2 * aug:width] = fc2_ref[layer]

    own = pl.ds(pl.multiple_of(me * rows, 16), rows)
    for layer in range(layers):
        g_ref[layer, own, :] = w_ref[layer]
    ones_row = (lax.broadcasted_iota(jnp.int32, (aug - model, TILE), 0) == 0).astype(F32).astype(BF16)
    for t in range(tiles):
        a_ref[t, model:, :] = ones_row
        o_ref[t, model:, :] = ones_row

    pl.semaphore_wait(barrier, len(neighbour) + 1)

    pieces = [(0, 0, aug), (0, aug, width - aug)] + [(layer, 0, width) for layer in range(1, layers)]

    def lanes_of(piece, part, parts):
        _, lo, size = pieces[piece]
        units = size // LANES
        first, last = -(-units * part // parts), -(-units * (part + 1) // parts)
        return pl.ds(lo + first * LANES, (last - first) * LANES)

    def slot(piece, dev, lanes):
        return g_ref.at[pieces[piece][0], pl.ds(pl.multiple_of(dev * rows, 16), rows), lanes]

    def relay(piece, m):
        step, part, offset, to, _ = MESSAGES[m]
        lanes = lanes_of(piece, *part)
        dst = slot(piece, device(offset), lanes)
        src = w_ref.at[pieces[piece][0], :, lanes] if step == 1 else dst
        return pltpu.make_async_remote_copy(
            src_ref=src, dst_ref=dst, send_sem=send_sem.at[piece, m], recv_sem=recv_sem.at[piece, m],
            device_id={"dp": neighbour[to]})

    def hand(piece, b):
        lanes = lanes_of(piece, 0, 1)
        if b == len(BLOCKS):
            src, dst = w_ref.at[pieces[piece][0], :, lanes], slot(piece, me, lanes)
        else:
            src = dst = slot(piece, device(BLOCKS[b]), lanes)
        return pltpu.make_async_remote_copy(
            src_ref=src, dst_ref=dst, send_sem=fsend_sem.at[piece, b], recv_sem=frecv_sem.at[piece, b],
            device_id={"dp": partner})

    def run(actions):
        for kind, piece, index in actions:
            if kind == "start":
                relay(piece, index).start()
            elif kind == "wait":
                relay(piece, index).wait_recv()
            else:
                hand(piece, index).start()

    def finish(piece):
        run(plan.hand_over(piece, everything=True))
        for b in range(len(BLOCKS) + 1):
            hand(piece, b).wait_recv()

    plan = Planner()
    run(plan.step(0, 1))

    zero_half = jnp.zeros((HEAD_DIM, TILE), BF16)
    for h in range(heads):
        other = HEAD_DIM * (1 - h % 2)
        for t in range(tiles):
            q_ref[h, t, other:other + HEAD_DIM, :] = zero_half
        extra = v_ref.shape[1] - HEAD_DIM
        v_ref[h, HEAD_DIM:, :] = (lax.broadcasted_iota(jnp.int32, (extra, v_ref.shape[2]), 0) == 0).astype(F32).astype(BF16)

    eye_m = eye(model)
    h_ref[tiles - 1, :, :] = jnp.zeros((model, TILE), BF16)
    fetch_x.wait()
    for t in range(tiles):
        size = min(TILE, frames - t * TILE)
        h_ref[t, :, 0:size] = mm_nt(eye_m, x_ref[t * TILE:t * TILE + size, :]).astype(BF16)

    run(plan.step(0, 2))
    run(plan.step(1, 1))

    def layer_norm(z, gain, shift):
        mean = jnp.sum(z, axis=0, keepdims=True) * (1.0 / model)
        c = z - mean
        var = jnp.sum(c * c, axis=0, keepdims=True) * (1.0 / model)
        return (c * lax.rsqrt(var + LN_EPSILON) * gain + shift).astype(BF16)

    def column(j, lane):
        return wa_ref[j, :, lane:lane + 1].astype(F32)

    def unpack(layer):
        block = 4 * HEAD_DIM
        row = lax.broadcasted_iota(jnp.int32, (block, block), 0)
        col = lax.broadcasted_iota(jnp.int32, (block, block), 1)
        perm = (col == lax.rem(row, HEAD_DIM) * 4 + row // HEAD_DIM).astype(F32).astype(BF16)
        for h in range(heads):
            mixed = mm(perm, g_ref[layer, h * block:(h + 1) * block, 0:aug]).astype(BF16)
            for j in range(4):
                wa_ref[j, h * HEAD_DIM:(h + 1) * HEAD_DIM, :] = mixed[j * HEAD_DIM:(j + 1) * HEAD_DIM]

    scale = HEAD_DIM ** -0.25
    half = TILE // 2
    eye_k = eye(TILE // 2)

    def pre(t):
        lanes = pl.ds(pl.multiple_of(t * TILE, TILE), TILE)
        a_ref[t, 0:model, :] = layer_norm(h_ref[t].astype(F32), column(0, model + 1), column(1, model + 1))
        a = a_ref[t]
        q = (mm(wa_ref[0], a) * scale).astype(BF16)
        for h in range(heads):
            lo = HEAD_DIM * (h % 2)
            q_ref[h, t, lo:lo + HEAD_DIM, :] = q[h * HEAD_DIM:(h + 1) * HEAD_DIM]
        kt = (mm(wa_ref[1], a) * scale).astype(BF16)
        for b in range(2):
            kn = mm_nt(eye_k, kt[:, b * half:(b + 1) * half]).astype(BF16)
            for p in range(pairs):
                k_ref[p, pl.ds(pl.multiple_of(t * TILE + b * half, half), half), :] = kn[:, p * LANES:(p + 1) * LANES]
        v = mm(wa_ref[2], a).astype(BF16)
        for h in range(heads):
            v_ref[h, 0:HEAD_DIM, lanes] = v[h * HEAD_DIM:(h + 1) * HEAD_DIM]

    s_refs, m_refs = (s0_ref, s1_ref), (m0_ref, m1_ref)

    def scores(p, hh, t, buf):
        s = mm(k_ref[p, 0:keys, :], q_ref[2 * p + hh, t])
        last = keys - 8
        row = lax.broadcasted_iota(jnp.int32, (8, TILE), 0) + last
        tail = jnp.where(row < frames, s[last:], -jnp.inf)
        s_refs[buf][0:last, :] = s[0:last]
        s_refs[buf][last:, :] = tail
        m_refs[buf][...] = jnp.maximum(jnp.max(s[0:last], axis=0, keepdims=True), jnp.max(tail, axis=0, keepdims=True))

    def values(p, hh, t, buf):
        h = 2 * p + hh
        e = jnp.exp(s_refs[buf][...] - m_refs[buf][...]).astype(BF16)
        o = mm(v_ref[h, :, 0:keys], e)
        inv = 1.0 / o[HEAD_DIM:HEAD_DIM + 1]
        o_ref[t, pl.ds(pl.multiple_of(h * HEAD_DIM, HEAD_DIM), HEAD_DIM), :] = (o[0:HEAD_DIM] * inv).astype(BF16)

    def attention(events):
        steps = [(hh, t) for hh in range(2) for t in range(tiles)]

        def body(p, carry):
            for j, (hh, t) in enumerate(steps):
                for (at, when), actions in events.items():
                    if when == j:
                        pl.when(p == at)(functools.partial(run, actions))
                scores(p, hh, t, j % 2)
                if j:
                    values(p, *steps[j - 1], (j - 1) % 2)
                else:
                    values(jnp.maximum(p - 1, 0), *steps[-1], 1)
            return carry

        lax.fori_loop(0, pairs, body, 0)
        values(pairs - 1, *steps[-1], 1)

    def unpack_mlp(layer):
        for b in range(hidden // TILE):
            w2 = g_ref[layer, b * TILE:(b + 1) * TILE, 2 * aug:2 * aug + model]
            w2t_ref[:, b * TILE:(b + 1) * TILE] = mm_nt(eye_m, w2).astype(BF16)

    def post(layer, t):
        r = h_ref[t].astype(F32) + mm(wa_ref[3], o_ref[t])
        r = r.astype(BF16)
        a_ref[t, 0:model, :] = layer_norm(r.astype(F32), column(2, model + 1), column(3, model + 1))
        c = a_ref[t]
        step = 2 * LANES
        for b in range(hidden // step):
            u = mm(g_ref[layer, b * step:(b + 1) * step, aug:2 * aug], c)
            z_ref[b * step:(b + 1) * step, :] = (0.5 * u * (1.0 + lax.erf(u * (2.0 ** -0.5)))).astype(BF16)
        y = r.astype(F32) + (mm(w2t_ref[...], z_ref[...]) + column(0, model + 2))
        h_ref[t] = y.astype(BF16)

    half = TILE // 2

    def out_copy(t):
        rows_out = pl.ds(pl.multiple_of(t * TILE, TILE), TILE)
        return pltpu.make_async_copy(y_ref.at[rows_out, :], out_hbm.at[rows_out, :], out_sem.at[t])

    def write_out(t):
        for b in range(2):
            y = mm_nt(eye_k, h_ref[t, :, b * half:(b + 1) * half]).astype(BF16)
            y_ref[pl.ds(pl.multiple_of(t * TILE + b * half, half), half), :] = y
        out_copy(t).start()

    for layer in range(layers):
        more = layer + 1 < layers
        if layer == 0:
            finish(0)
        unpack(layer)
        lax.fori_loop(0, tiles, lambda t, c: (pre(t), c)[1], 0)
        events = {}
        if layer == 0:
            events[0, 3] = plan.step(1, 2)
        if more:
            events.setdefault((0, 3), []).extend(plan.step(layer + 2, 1))
            if layer == 0:
                events[2, 0] = plan.hand_over(1, everything=True)
            events[2, 3] = plan.step(layer + 2, 2)
        attention(events)
        if layer == 0:
            finish(1)
        unpack_mlp(layer)
        finals = not more
        late = plan.hand_over(layer + 2, everything=True) if more else []

        def tile(t, carry, layer=layer, late=late):
            if late:
                pl.when(t == 1)(functools.partial(run, late))
            post(layer, t)
            if finals:
                write_out(t)
            return carry

        lax.fori_loop(0, tiles, tile, 0)
        if more:
            finish(layer + 2)

    for t in range(tiles):
        out_copy(t).wait()

    for piece in range(len(pieces)):
        for m in range(len(MESSAGES)):
            relay(piece, m).wait_send()
        for b in range(len(BLOCKS) + 1):
            hand(piece, b).wait_send()


def solution(mesh):
    n = mesh.shape["dp"]

    def body(audio_x, attn_w, fc1_w, fc2_w, vec_d, b1_vec):
        layers, four, model, cols = attn_w.shape
        hidden_cols = fc1_w.shape[2]
        batch, frames, _ = audio_x.shape
        hidden = hidden_cols * n
        aug = model + LANES
        rows = four * cols
        attn = jnp.transpose(attn_w, (0, 3, 1, 2))
        fc1 = jnp.transpose(fc1_w, (0, 2, 1))

        tiles = -(-frames // TILE)
        padded = tiles * TILE
        keys = -(-frames // 16) * 16
        heads = model // HEAD_DIM
        pieces = layers + 1
        vmem = pl.BlockSpec(memory_space=pltpu.VMEM)
        out = pl.pallas_call(
            functools.partial(kernel, n),
            out_shape=jax.ShapeDtypeStruct((padded, model), audio_x.dtype),
            in_specs=[pl.BlockSpec(memory_space=pl.ANY)] + [vmem] * 5,
            out_specs=pl.BlockSpec(memory_space=pl.ANY),
            scratch_shapes=[
                pltpu.VMEM((layers, rows, 2 * aug + model), BF16),
                pltpu.VMEM((rows, model), F32),
                pltpu.VMEM((layers, n * rows, 2 * aug + model), BF16),
                pltpu.VMEM((four, model, aug), BF16),
                pltpu.VMEM((model, hidden), BF16),
                pltpu.VMEM((frames, model), BF16),
                pltpu.VMEM((padded, model), BF16),
                pltpu.VMEM((tiles, model, TILE), BF16),
                pltpu.VMEM((tiles, aug, TILE), BF16),
                pltpu.VMEM((heads, tiles, LANES, TILE), BF16),
                pltpu.VMEM((heads // 2, padded, LANES), BF16),
                pltpu.VMEM((heads, HEAD_DIM + 16, padded), BF16),
                pltpu.VMEM((tiles, aug, TILE), BF16),
                pltpu.VMEM((hidden, TILE), BF16),
                pltpu.VMEM((keys, TILE), F32),
                pltpu.VMEM((keys, TILE), F32),
                pltpu.VMEM((1, TILE), F32),
                pltpu.VMEM((1, TILE), F32),
                pltpu.SemaphoreType.DMA,
                pltpu.SemaphoreType.DMA((tiles,)),
                pltpu.SemaphoreType.DMA((pieces, len(MESSAGES))),
                pltpu.SemaphoreType.DMA((pieces, len(MESSAGES))),
                pltpu.SemaphoreType.DMA((pieces, len(BLOCKS) + 1)),
                pltpu.SemaphoreType.DMA((pieces, len(BLOCKS) + 1)),
            ],
            compiler_params=pltpu.CompilerParams(
                collective_id=0, has_side_effects=True, vmem_limit_bytes=60 * 1024 * 1024),
        )(audio_x, attn, fc1, fc2_w, vec_d, b1_vec)
        return out[None, :frames]

    return jax.shard_map(
        body, mesh=mesh,
        in_specs=(P(('rep', 'dp')), P(None, None, None, 'dp'), P(None, None, 'dp'), P(None, 'dp', None), P(None, None, 'dp'), P(None, 'dp')),
        out_specs=P(('rep', 'dp')), check_vma=False)
```

```python
import functools

import jax
import jax.numpy as jnp
from jax import lax
from jax.experimental import pallas as pl
from jax.experimental.pallas import tpu as pltpu
from jax.sharding import PartitionSpec as P

HEAD_DIM = 64
LN_EPSILON = 1e-5
LANES = 128
TILE = 512
KEY_BLOCK = 256
LAG = 2
F32, BF16 = jnp.float32, jnp.bfloat16
NT = (((1,), (1,)), ((), ()))


def mm(a, b):
    return jnp.dot(a, b, preferred_element_type=F32)


def mm_nt(a, b):
    return lax.dot_general(a, b, NT, preferred_element_type=F32)


def eye(n):
    row = lax.broadcasted_iota(jnp.int32, (n, n), 0)
    col = lax.broadcasted_iota(jnp.int32, (n, n), 1)
    return (row == col).astype(F32).astype(BF16)


RING = 4


def relay_plan():
    messages, complete = [], {}

    def add(*message):
        messages.append(message)
        return len(messages) - 1

    def at(a, b):
        return a % RING, b % RING

    both = (1, -1)
    axes = [(1, 0), (-1, 0), (0, 1), (0, -1)]
    corners = [(a, b) for a in both for b in both]
    own = {to: add(1, (0, 1), at(0, 0), to, ()) for to in axes + corners}
    for (a, b), m in own.items():
        complete[at(-a, -b)] = (m,)
    for part, s in enumerate(both):
        for r in (0, 1, -1):
            m = add(2, (part, 2), at(-s, -r), (s, 0), (own[s, r],))
            complete[at(2, -r)] = complete.get(at(2, -r), ()) + (m,)
            m = add(2, (part, 2), at(-r, -s), (0, s), (own[r, s],))
            complete[at(-r, 2)] = complete.get(at(-r, 2), ()) + (m,)
    for part, (a, b) in enumerate(corners):
        m = add(2, (part, 4), at(-a, -b), (a, b), (own[a, b],))
        complete[at(2, 2)] = complete.get(at(2, 2), ()) + (m,)
    return messages, complete


MESSAGES, COMPLETE = relay_plan()
BLOCKS = list(COMPLETE)


class Planner:
    def __init__(self):
        self.arrived, self.passed = set(), set()

    def step(self, piece, step):
        actions = []
        for m, message in enumerate(MESSAGES):
            if message[0] == step:
                actions += self.need(piece, message[-1])
                actions.append(("start", piece, m))
        if step == 1 and piece == 0:
            actions.append(("pass", piece, len(BLOCKS)))
        return actions + self.hand_over(piece)

    def need(self, piece, deps):
        actions = [("wait", piece, m) for m in deps if (piece, m) not in self.arrived]
        self.arrived.update((piece, m) for m in deps)
        return actions

    def hand_over(self, piece, everything=False):
        if piece:
            if not everything or (piece, "all") in self.passed:
                return []
            self.passed.add((piece, "all"))
            return self.need(piece, range(len(MESSAGES))) + [("pass", piece, len(BLOCKS))]
        actions = []
        for b, block in enumerate(BLOCKS):
            if (piece, b) in self.passed:
                continue
            if everything:
                actions += self.need(piece, COMPLETE[block])
            if all((piece, m) in self.arrived for m in COMPLETE[block]):
                actions.append(("pass", piece, b))
                self.passed.add((piece, b))
        if everything:
            actions += self.need(piece, range(len(MESSAGES)))
        return actions


def kernel(n, x_hbm, attn_ref, fc1_ref, fc2_ref, vec_ref, b1_ref, out_hbm, w_ref, row_ref, g_ref, wa_ref, w2t_ref, x_ref, y_ref, h_ref, a_ref,
           q_ref, k_ref, v_ref, o_ref, z_ref, s0_ref, s1_ref, m0_ref, m1_ref, acc_ref, x_sem, out_sem, send_sem, recv_sem, fsend_sem, frecv_sem):
    layers, rows, width = w_ref.shape
    _, frames, model = x_hbm.shape
    aug = wa_ref.shape[2]
    heads = model // HEAD_DIM
    pairs = heads // 2
    hidden = z_ref.shape[0]
    tiles = h_ref.shape[0]
    keys = s0_ref.shape[0]

    fetch_x = pltpu.make_async_copy(x_hbm.at[0], x_ref, x_sem)
    fetch_x.start()

    me = lax.axis_index("dp")
    core = lax.rem(me, 2)
    chip = me // 2
    chip_x, chip_y = lax.rem(chip, RING), chip // RING

    def device(offset):
        x = lax.rem(chip_x + offset[0] + RING, RING)
        y = lax.rem(chip_y + offset[1] + RING, RING)
        return 2 * (y * RING + x) + core

    partner = me + 1 - 2 * core
    neighbour = {to: device(to) for step, _, _, to, _ in MESSAGES if step == 1}

    barrier = pltpu.get_barrier_semaphore()
    for dev in [*neighbour.values(), partner]:
        pl.semaphore_signal(barrier, inc=1, device_id={"dp": dev})

    def pick(layer, want):
        row = lax.broadcasted_iota(jnp.int32, (rows, vec_ref.shape[1]), 0)
        col = lax.broadcasted_iota(jnp.int32, (rows, vec_ref.shape[1]), 1)
        sel = jnp.zeros(row.shape, F32)
        for j, r in enumerate(want):
            if r is not None:
                sel = jnp.where((lax.rem(row, 4) == j) & (col == r), 1.0, sel)
        spread = mm(sel, vec_ref[layer].astype(F32))
        row = lax.broadcasted_iota(jnp.int32, spread.shape, 0)
        col = lax.broadcasted_iota(jnp.int32, spread.shape, 1)
        return jnp.sum(jnp.where(row // 4 == col, spread, 0.0), axis=1, keepdims=True)

    lane = lax.broadcasted_iota(jnp.int32, (rows, LANES), 1)
    for layer in range(layers):
        for c in range(rows // 4):
            row_ref[4 * c:4 * c + 4, :] = attn_ref[layer, c].astype(F32)
        w_ref[layer, :, 0:model] = row_ref[...].astype(BF16)
        entry = [pick(layer, want) for want in ((0, None, 1, 2), (4, 5, 6, 7), (3, None, None, None))]
        extra = jnp.where(lane == 0, entry[0], jnp.where(lane == 1, entry[1], jnp.where(lane == 2, entry[2], 0.0)))
        w_ref[layer, :, model:aug] = extra.astype(BF16)
        w_ref[layer, :, aug:aug + model] = fc1_ref[layer]
        row = lax.broadcasted_iota(jnp.int32, (rows, rows), 0)
        col = lax.broadcasted_iota(jnp.int32, (rows, rows), 1)
        b1 = jnp.sum(jnp.where(row == col, b1_ref[layer:layer + 1, :].astype(F32), 0.0), axis=1, keepdims=True)
        w_ref[layer, :, aug + model:2 * aug] = jnp.where(lane == 0, b1, 0.0).astype(BF16)
        w_ref[layer, :, 2 * aug:width] = fc2_ref[layer]

    own = pl.ds(pl.multiple_of(me * rows, 16), rows)
    for layer in range(layers):
        g_ref[layer, own, :] = w_ref[layer]
    ones_row = (lax.broadcasted_iota(jnp.int32, (aug - model, TILE), 0) == 0).astype(F32).astype(BF16)
    for t in range(tiles):
        a_ref[t, model:, :] = ones_row
        o_ref[t, model:, :] = ones_row

    pl.semaphore_wait(barrier, len(neighbour) + 1)

    pieces = [piece for layer in range(layers) for piece in ((layer, 0, aug), (layer, aug, width - aug))]

    def lanes_of(piece, part, parts):
        _, lo, size = pieces[piece]
        units = size // LANES
        first, last = -(-units * part // parts), -(-units * (part + 1) // parts)
        return pl.ds(lo + first * LANES, (last - first) * LANES)

    def slot(piece, dev, lanes):
        return g_ref.at[pieces[piece][0], pl.ds(pl.multiple_of(dev * rows, 16), rows), lanes]

    def relay(piece, m):
        step, part, offset, to, _ = MESSAGES[m]
        lanes = lanes_of(piece, *part)
        dst = slot(piece, device(offset), lanes)
        src = w_ref.at[pieces[piece][0], :, lanes] if step == 1 else dst
        return pltpu.make_async_remote_copy(
            src_ref=src, dst_ref=dst, send_sem=send_sem.at[piece, m], recv_sem=recv_sem.at[piece, m],
            device_id={"dp": neighbour[to]})

    def hand(piece, b):
        lanes = lanes_of(piece, 0, 1)
        if piece:
            src = dst = g_ref.reshape(layers, n // 2, 2, rows, width).at[pieces[piece][0], :, core, :, lanes]
        elif b == len(BLOCKS):
            src, dst = w_ref.at[pieces[piece][0], :, lanes], slot(piece, me, lanes)
        else:
            src = dst = slot(piece, device(BLOCKS[b]), lanes)
        return pltpu.make_async_remote_copy(
            src_ref=src, dst_ref=dst, send_sem=fsend_sem.at[piece, b], recv_sem=frecv_sem.at[piece, b],
            device_id={"dp": partner})

    def run(actions):
        for kind, piece, index in actions:
            if kind == "start":
                relay(piece, index).start()
            elif kind == "wait":
                relay(piece, index).wait_recv()
            else:
                hand(piece, index).start()

    def finish(piece):
        run(plan.hand_over(piece, everything=True))
        for b in handed(piece):
            hand(piece, b).wait_recv()

    def handed(piece):
        return range(len(BLOCKS) + 1) if piece == 0 else [len(BLOCKS)]

    plan = Planner()
    run(plan.step(0, 1))

    zero_half = jnp.zeros((HEAD_DIM, TILE), BF16)
    for h in range(heads):
        other = HEAD_DIM * (1 - h % 2)
        for t in range(tiles):
            q_ref[h, t, other:other + HEAD_DIM, :] = zero_half
        extra = v_ref.shape[1] - HEAD_DIM
        v_ref[h, HEAD_DIM:, :] = (lax.broadcasted_iota(jnp.int32, (extra, v_ref.shape[2]), 0) == 0).astype(F32).astype(BF16)

    eye_m = eye(model)
    h_ref[tiles - 1, :, :] = jnp.zeros((model, TILE), BF16)
    fetch_x.wait()
    for t in range(tiles):
        size = min(TILE, frames - t * TILE)
        h_ref[t, :, 0:size] = mm_nt(eye_m, x_ref[t * TILE:t * TILE + size, :]).astype(BF16)

    run(plan.step(0, 2))
    run(plan.step(1, 1))
    if layers > 1:
        run(plan.step(2, 1))

    def layer_norm(z, gain, shift):
        mean = jnp.sum(z, axis=0, keepdims=True) * (1.0 / model)
        c = z - mean
        var = jnp.sum(c * c, axis=0, keepdims=True) * (1.0 / model)
        return (c * lax.rsqrt(var + LN_EPSILON) * gain + shift).astype(BF16)

    def column(j, lane):
        return wa_ref[j, :, lane:lane + 1].astype(F32)

    def unpack(layer):
        block = 4 * HEAD_DIM
        row = lax.broadcasted_iota(jnp.int32, (block, block), 0)
        col = lax.broadcasted_iota(jnp.int32, (block, block), 1)
        perm = (col == lax.rem(row, HEAD_DIM) * 4 + row // HEAD_DIM).astype(F32).astype(BF16)
        for h in range(heads):
            mixed = mm(perm, g_ref[layer, h * block:(h + 1) * block, 0:aug]).astype(BF16)
            for j in range(4):
                wa_ref[j, h * HEAD_DIM:(h + 1) * HEAD_DIM, :] = mixed[j * HEAD_DIM:(j + 1) * HEAD_DIM]

    scale = HEAD_DIM ** -0.25
    half = TILE // 2
    eye_k = eye(TILE // 2)

    def norm(t, which):
        gain, shift = column(which, model + 1), column(which + 1, model + 1)
        a_ref[t, 0:model, :] = layer_norm(h_ref[t].astype(F32), gain, shift)

    def project(t):
        a = a_ref[t]
        kt = (mm(wa_ref[1], a) * scale).astype(BF16)
        q = (mm(wa_ref[0], a) * scale).astype(BF16)
        for h in range(heads):
            lo = HEAD_DIM * (h % 2)
            q_ref[h, t, lo:lo + HEAD_DIM, :] = q[h * HEAD_DIM:(h + 1) * HEAD_DIM]
        v = mm(wa_ref[2], a).astype(BF16)
        for h in range(heads):
            v_ref[h, 0:HEAD_DIM, t * TILE:(t + 1) * TILE] = v[h * HEAD_DIM:(h + 1) * HEAD_DIM]
        for b in range(2):
            kn = mm_nt(eye_k, kt[:, b * half:(b + 1) * half]).astype(BF16)
            for p in range(pairs):
                k_ref[p, t * TILE + b * half:t * TILE + (b + 1) * half, :] = kn[:, p * LANES:(p + 1) * LANES]

    def pre():
        norm(0, 0)
        for t in range(tiles):
            if t + 1 < tiles:
                norm(t + 1, 0)
            project(t)

    s_refs, m_refs = (s0_ref, s1_ref), (m0_ref, m1_ref)

    blocks = [(lo, min(KEY_BLOCK, keys - lo)) for lo in range(0, keys, KEY_BLOCK)]
    steps = [(hh, t) for hh in range(2) for t in range(tiles)]

    def scores(p, j, c, top):
        (hh, t), (lo, size) = steps[j], blocks[c]
        s_ref = s_refs[j % 2]
        s = mm(k_ref[p, lo:lo + size, :], q_ref[2 * p + hh, t])
        whole = size
        if lo + size > frames:
            whole = size - 8
            row = lax.broadcasted_iota(jnp.int32, (8, TILE), 0) + (lo + whole)
            tail = jnp.where(row < frames, s[whole:], -jnp.inf)
            s_ref[lo + whole:lo + size, :] = tail
            top = jnp.maximum(top, tail)
        s_ref[lo:lo + whole, :] = s[0:whole]
        high = jnp.max(s[0:whole].reshape(whole // 8, 8, TILE), axis=0)
        top = high if top is None else jnp.maximum(top, high)
        if c == len(blocks) - 1:
            m_refs[j % 2][...] = jnp.max(top, axis=0, keepdims=True)
        return top

    def values(p, j, c, total):
        (hh, t), (lo, size) = steps[j], blocks[c]
        h = 2 * p + hh
        e = jnp.exp(s_refs[j % 2][lo:lo + size, :] - m_refs[j % 2][...]).astype(BF16)
        part = mm(v_ref[h, :, lo:lo + size], e)
        total = part if c == 0 else total + part
        if c == len(blocks) - 1:
            inv = 1.0 / total[HEAD_DIM:HEAD_DIM + 1]
            o_ref[t, pl.ds(pl.multiple_of(h * HEAD_DIM, HEAD_DIM), HEAD_DIM), :] = (total[0:HEAD_DIM] * inv).astype(BF16)
        return total

    def attention(events):
        count = len(blocks)

        def body(p, carry):
            total = acc_ref[...]
            for j in range(len(steps)):
                for (at, when), actions in events.items():
                    if when == j:
                        pl.when(p == at)(functools.partial(run, actions))
                top = None
                for c in range(count):
                    top = scores(p, j, c, top)
                    back, at = divmod(j * count + c - LAG - count, count)
                    if back < 0:
                        total = values(jnp.maximum(p - 1, 0), back + len(steps), at, total)
                    else:
                        total = values(p, back, at, total)
            acc_ref[...] = total
            return carry

        lax.fori_loop(0, pairs, body, 0)
        total = acc_ref[...]
        for k in range(len(steps) * count - LAG - count, len(steps) * count):
            total = values(pairs - 1, *divmod(k, count), total)

    def unpack_mlp(layer):
        for b in range(hidden // TILE):
            w2 = g_ref[layer, b * TILE:(b + 1) * TILE, 2 * aug:2 * aug + model]
            w2t_ref[:, b * TILE:(b + 1) * TILE] = mm_nt(eye_m, w2).astype(BF16)

    def out_project(t):
        r = h_ref[t].astype(F32) + mm(wa_ref[3], o_ref[t])
        h_ref[t] = r.astype(BF16)

    def mlp(layer, t):
        c = a_ref[t]
        step = 2 * LANES
        for b in range(hidden // step):
            u = mm(g_ref[layer, b * step:(b + 1) * step, aug:2 * aug], c)
            z_ref[b * step:(b + 1) * step, :] = (0.5 * u * (1.0 + lax.erf(u * (2.0 ** -0.5)))).astype(BF16)
        y = h_ref[t].astype(F32) + (mm(w2t_ref[...], z_ref[...]) + column(0, model + 2))
        h_ref[t] = y.astype(BF16)

    def out_copy(t):
        rows_out = pl.ds(pl.multiple_of(t * TILE, TILE), TILE)
        return pltpu.make_async_copy(y_ref.at[rows_out, :], out_hbm.at[rows_out, :], out_sem.at[t])

    def write_out(t):
        for b in range(2):
            y = mm_nt(eye_k, h_ref[t, :, b * half:(b + 1) * half]).astype(BF16)
            y_ref[pl.ds(pl.multiple_of(t * TILE + b * half, half), half), :] = y
        out_copy(t).start()

    for layer in range(layers):
        more = layer + 1 < layers
        if layer == 0:
            finish(0)
        unpack(layer)
        pre()
        this, after = 2 * layer + 1, 2 * layer + 2
        events = {(0, 0): plan.step(this, 2) if layer == 0 else plan.hand_over(this, everything=True)}
        if more:
            if layer:
                events[0, 0] += plan.step(after, 1)
            events[0, 3] = plan.step(after, 2) + plan.step(after + 1, 1)
        if layer == 0:
            events[pairs - 1, 0] = plan.hand_over(this, everything=True)
        if more:
            events[pairs - 1, 3] = plan.hand_over(after, everything=True)
        attention(events)
        finish(this)
        if more:
            run(plan.step(after + 1, 2))
        out_project(0)
        unpack_mlp(layer)
        for t in range(tiles):
            if t + 1 < tiles:
                out_project(t + 1)
            norm(t, 2)

        def tile(t, carry, layer=layer, more=more):
            mlp(layer, t)
            if not more:
                write_out(t)
            return carry

        lax.fori_loop(0, tiles, tile, 0)
        if more:
            finish(after)

    for t in range(tiles):
        out_copy(t).wait()

    for piece in range(len(pieces)):
        for m in range(len(MESSAGES)):
            relay(piece, m).wait_send()
        for b in handed(piece):
            hand(piece, b).wait_send()


def solution(mesh):
    n = mesh.shape["dp"]

    def body(audio_x, attn_w, fc1_w, fc2_w, vec_d, b1_vec):
        layers, four, model, cols = attn_w.shape
        hidden_cols = fc1_w.shape[2]
        batch, frames, _ = audio_x.shape
        hidden = hidden_cols * n
        aug = model + LANES
        rows = four * cols
        attn = jnp.transpose(attn_w, (0, 3, 1, 2))
        fc1 = jnp.transpose(fc1_w, (0, 2, 1))

        tiles = -(-frames // TILE)
        padded = tiles * TILE
        keys = -(-frames // 16) * 16
        heads = model // HEAD_DIM
        pieces = 2 * layers
        vmem = pl.BlockSpec(memory_space=pltpu.VMEM)
        out = pl.pallas_call(
            functools.partial(kernel, n),
            out_shape=jax.ShapeDtypeStruct((padded, model), audio_x.dtype),
            in_specs=[pl.BlockSpec(memory_space=pl.ANY)] + [vmem] * 5,
            out_specs=pl.BlockSpec(memory_space=pl.ANY),
            scratch_shapes=[
                pltpu.VMEM((layers, rows, 2 * aug + model), BF16),
                pltpu.VMEM((rows, model), F32),
                pltpu.VMEM((layers, n * rows, 2 * aug + model), BF16),
                pltpu.VMEM((four, model, aug), BF16),
                pltpu.VMEM((model, hidden), BF16),
                pltpu.VMEM((frames, model), BF16),
                pltpu.VMEM((padded, model), BF16),
                pltpu.VMEM((tiles, model, TILE), BF16),
                pltpu.VMEM((tiles, aug, TILE), BF16),
                pltpu.VMEM((heads, tiles, LANES, TILE), BF16),
                pltpu.VMEM((heads // 2, padded, LANES), BF16),
                pltpu.VMEM((heads, HEAD_DIM + 16, padded), BF16),
                pltpu.VMEM((tiles, aug, TILE), BF16),
                pltpu.VMEM((hidden, TILE), BF16),
                pltpu.VMEM((keys, TILE), F32),
                pltpu.VMEM((keys, TILE), F32),
                pltpu.VMEM((1, TILE), F32),
                pltpu.VMEM((1, TILE), F32),
                pltpu.VMEM((HEAD_DIM + 16, TILE), F32),
                pltpu.SemaphoreType.DMA,
                pltpu.SemaphoreType.DMA((tiles,)),
                pltpu.SemaphoreType.DMA((pieces, len(MESSAGES))),
                pltpu.SemaphoreType.DMA((pieces, len(MESSAGES))),
                pltpu.SemaphoreType.DMA((pieces, len(BLOCKS) + 1)),
                pltpu.SemaphoreType.DMA((pieces, len(BLOCKS) + 1)),
            ],
            compiler_params=pltpu.CompilerParams(
                collective_id=0, has_side_effects=True, vmem_limit_bytes=60 * 1024 * 1024),
        )(audio_x, attn, fc1, fc2_w, vec_d, b1_vec)
        return out[None, :frames]

    return jax.shard_map(
        body, mesh=mesh,
        in_specs=(P(('rep', 'dp')), P(None, None, None, 'dp'), P(None, None, 'dp'), P(None, 'dp', None), P(None, None, 'dp'), P(None, 'dp')),
        out_specs=P(('rep', 'dp')), check_vma=False)
```

```python
import functools

import jax
import jax.numpy as jnp
from jax import lax
from jax.experimental import pallas as pl
from jax.experimental.pallas import tpu as pltpu
from jax.sharding import PartitionSpec as P

HEAD_DIM = 64
LN_EPSILON = 1e-5
LANES = 128
TILE = 512
KEY_BLOCK = 256
LAG = 2
F32, BF16 = jnp.float32, jnp.bfloat16
NT = (((1,), (1,)), ((), ()))


def mm(a, b):
    return jnp.dot(a, b, preferred_element_type=F32)


def mm_nt(a, b):
    return lax.dot_general(a, b, NT, preferred_element_type=F32)


def eye(n):
    row = lax.broadcasted_iota(jnp.int32, (n, n), 0)
    col = lax.broadcasted_iota(jnp.int32, (n, n), 1)
    return (row == col).astype(F32).astype(BF16)


RING = 4


def relay_plan():
    messages, complete = [], {}

    def add(*message):
        messages.append(message)
        return len(messages) - 1

    def at(a, b):
        return a % RING, b % RING

    both = (1, -1)
    axes = [(1, 0), (-1, 0), (0, 1), (0, -1)]
    corners = [(a, b) for a in both for b in both]
    own = {to: add(1, (0, 1), at(0, 0), to, ()) for to in axes + corners}
    for (a, b), m in own.items():
        complete[at(-a, -b)] = (m,)
    for part, s in enumerate(both):
        for r in (0, 1, -1):
            m = add(2, (part, 2), at(-s, -r), (s, 0), (own[s, r],))
            complete[at(2, -r)] = complete.get(at(2, -r), ()) + (m,)
            m = add(2, (part, 2), at(-r, -s), (0, s), (own[r, s],))
            complete[at(-r, 2)] = complete.get(at(-r, 2), ()) + (m,)
    for part, (a, b) in enumerate(corners):
        m = add(2, (part, 4), at(-a, -b), (a, b), (own[a, b],))
        complete[at(2, 2)] = complete.get(at(2, 2), ()) + (m,)
    return messages, complete


MESSAGES, COMPLETE = relay_plan()
BLOCKS = list(COMPLETE)


class Planner:
    def __init__(self):
        self.arrived, self.passed = set(), set()

    def step(self, piece, step):
        actions = []
        for m, message in enumerate(MESSAGES):
            if message[0] == step:
                actions += self.need(piece, message[-1])
                actions.append(("start", piece, m))
        if step == 1 and piece == 0:
            actions.append(("pass", piece, len(BLOCKS)))
        return actions + self.hand_over(piece)

    def need(self, piece, deps):
        actions = [("wait", piece, m) for m in deps if (piece, m) not in self.arrived]
        self.arrived.update((piece, m) for m in deps)
        return actions

    def hand_over(self, piece, everything=False):
        if piece:
            if not everything or (piece, "all") in self.passed:
                return []
            self.passed.add((piece, "all"))
            return self.need(piece, range(len(MESSAGES))) + [("pass", piece, len(BLOCKS))]
        actions = []
        for b, block in enumerate(BLOCKS):
            if (piece, b) in self.passed:
                continue
            if everything:
                actions += self.need(piece, COMPLETE[block])
            if all((piece, m) in self.arrived for m in COMPLETE[block]):
                actions.append(("pass", piece, b))
                self.passed.add((piece, b))
        if everything:
            actions += self.need(piece, range(len(MESSAGES)))
        return actions


def kernel(n, x_hbm, attn_hbm, fc1_hbm, fc2_hbm, vec_hbm, b1_hbm, out_hbm, attn_ref, fc1_ref, fc2_ref, vec_ref, b1_ref, w_ref, row_ref, g_ref, wa_ref, w2t_ref, x_ref, y_ref, h_ref, a_ref,
           q_ref, k_ref, v_ref, o_ref, z_ref, s0_ref, s1_ref, m0_ref, m1_ref, acc_ref, x_sem, out_sem, send_sem, recv_sem, fsend_sem, frecv_sem):
    layers, rows, width = w_ref.shape
    _, frames, model = x_hbm.shape
    aug = wa_ref.shape[3]
    heads = model // HEAD_DIM
    pairs = heads // 2
    hidden = z_ref.shape[0]
    tiles = h_ref.shape[0]
    keys = s0_ref.shape[0]

    me = lax.axis_index("dp")
    core = lax.rem(me, 2)
    chip = me // 2
    chip_x, chip_y = lax.rem(chip, RING), chip // RING

    @functools.cache
    def device(offset):
        x = lax.rem(chip_x + offset[0] + RING, RING)
        y = lax.rem(chip_y + offset[1] + RING, RING)
        return 2 * (y * RING + x) + core

    partner = me + 1 - 2 * core
    neighbour = {to: device((to[0] % RING, to[1] % RING)) for step, _, _, to, _ in MESSAGES if step == 1}
    for offset in BLOCKS + [(0, 0)]:
        device(offset)

    barrier = pltpu.get_barrier_semaphore()
    for dev in [*neighbour.values(), partner]:
        pl.semaphore_signal(barrier, inc=1, device_id={"dp": dev})

    fetches = [pltpu.make_async_copy(src, dst, x_sem.at[i]) for i, (src, dst) in enumerate([
        (attn_hbm, attn_ref), (vec_hbm, vec_ref), (fc1_hbm, fc1_ref), (fc2_hbm, fc2_ref), (b1_hbm, b1_ref), (x_hbm.at[0], x_ref)])]
    for fetch in fetches:
        fetch.start()
    fetch_x = fetches.pop()

    ones_row = (lax.broadcasted_iota(jnp.int32, (aug - model, TILE), 0) == 0).astype(F32).astype(BF16)
    for t in range(tiles):
        a_ref[t, model:, :] = ones_row
        o_ref[t, model:, :] = ones_row
    for fetch in fetches:
        fetch.wait()

    def pick(layer, want):
        row = lax.broadcasted_iota(jnp.int32, (rows, vec_ref.shape[1]), 0)
        col = lax.broadcasted_iota(jnp.int32, (rows, vec_ref.shape[1]), 1)
        sel = jnp.zeros(row.shape, F32)
        for j, r in enumerate(want):
            if r is not None:
                sel = jnp.where((lax.rem(row, 4) == j) & (col == r), 1.0, sel)
        spread = mm(sel, vec_ref[layer].astype(F32))
        row = lax.broadcasted_iota(jnp.int32, spread.shape, 0)
        col = lax.broadcasted_iota(jnp.int32, spread.shape, 1)
        return jnp.sum(jnp.where(row // 4 == col, spread, 0.0), axis=1, keepdims=True)

    lane = lax.broadcasted_iota(jnp.int32, (rows, LANES), 1)
    for layer in range(layers):
        for c in range(rows // 4):
            row_ref[4 * c:4 * c + 4, :] = attn_ref[layer, c].astype(F32)
        w_ref[layer, :, 0:model] = row_ref[...].astype(BF16)
        entry = [pick(layer, want) for want in ((0, None, 1, 2), (4, 5, 6, 7), (3, None, None, None))]
        extra = jnp.where(lane == 0, entry[0], jnp.where(lane == 1, entry[1], jnp.where(lane == 2, entry[2], 0.0)))
        w_ref[layer, :, model:aug] = extra.astype(BF16)
        w_ref[layer, :, aug:aug + model] = fc1_ref[layer]
        row = lax.broadcasted_iota(jnp.int32, (rows, rows), 0)
        col = lax.broadcasted_iota(jnp.int32, (rows, rows), 1)
        b1 = jnp.sum(jnp.where(row == col, b1_ref[layer:layer + 1, :].astype(F32), 0.0), axis=1, keepdims=True)
        w_ref[layer, :, aug + model:2 * aug] = jnp.where(lane == 0, b1, 0.0).astype(BF16)
        w_ref[layer, :, 2 * aug:width] = fc2_ref[layer]

    own = pl.ds(pl.multiple_of(me * rows, 16), rows)
    for layer in range(layers):
        g_ref[layer, own, :] = w_ref[layer]
    pl.semaphore_wait(barrier, len(neighbour) + 1)

    pieces = [piece for layer in range(layers) for piece in ((layer, 0, aug), (layer, aug, width - aug))]

    def lanes_of(piece, part, parts):
        _, lo, size = pieces[piece]
        units = size // LANES
        first, last = -(-units * part // parts), -(-units * (part + 1) // parts)
        return pl.ds(lo + first * LANES, (last - first) * LANES)

    def slot(piece, dev, lanes):
        return g_ref.at[pieces[piece][0], pl.ds(pl.multiple_of(dev * rows, 16), rows), lanes]

    def relay(piece, m):
        step, part, offset, to, _ = MESSAGES[m]
        lanes = lanes_of(piece, *part)
        dst = slot(piece, device(offset), lanes)
        src = w_ref.at[pieces[piece][0], :, lanes] if step == 1 else dst
        return pltpu.make_async_remote_copy(
            src_ref=src, dst_ref=dst, send_sem=send_sem.at[piece, m], recv_sem=recv_sem.at[piece, m],
            device_id={"dp": neighbour[to]})

    def hand(piece, b):
        lanes = lanes_of(piece, 0, 1)
        if piece:
            src = dst = g_ref.reshape(layers, n // 2, 2, rows, width).at[pieces[piece][0], :, core, :, lanes]
        elif b == len(BLOCKS):
            src, dst = w_ref.at[pieces[piece][0], :, lanes], slot(piece, me, lanes)
        else:
            src = dst = slot(piece, device(BLOCKS[b]), lanes)
        return pltpu.make_async_remote_copy(
            src_ref=src, dst_ref=dst, send_sem=fsend_sem.at[piece, b], recv_sem=frecv_sem.at[piece, b],
            device_id={"dp": partner})

    def run(actions):
        for kind, piece, index in actions:
            if kind == "start":
                relay(piece, index).start()
            elif kind == "wait":
                relay(piece, index).wait_recv()
            else:
                hand(piece, index).start()

    def finish(piece):
        run(plan.hand_over(piece, everything=True))
        for b in handed(piece):
            hand(piece, b).wait_recv()

    def handed(piece):
        return range(len(BLOCKS) + 1) if piece == 0 else [len(BLOCKS)]

    plan = Planner()
    run(plan.step(0, 1))

    zero_half = jnp.zeros((HEAD_DIM, TILE), BF16)
    for h in range(heads):
        other = HEAD_DIM * (1 - h % 2)
        for t in range(tiles):
            q_ref[h, t, other:other + HEAD_DIM, :] = zero_half
        extra = v_ref.shape[1] - HEAD_DIM
        v_ref[h, HEAD_DIM:, :] = (lax.broadcasted_iota(jnp.int32, (extra, v_ref.shape[2]), 0) == 0).astype(F32).astype(BF16)

    eye_m = eye(model)
    h_ref[tiles - 1, :, :] = jnp.zeros((model, TILE), BF16)
    fetch_x.wait()
    for t in range(tiles):
        size = min(TILE, frames - t * TILE)
        h_ref[t, :, 0:size] = mm_nt(eye_m, x_ref[t * TILE:t * TILE + size, :]).astype(BF16)

    run(plan.step(0, 2))
    run(plan.step(1, 1))
    if layers > 1:
        run(plan.step(2, 1))

    def layer_norm(z, gain, shift):
        mean = jnp.sum(z, axis=0, keepdims=True) * (1.0 / model)
        c = z - mean
        var = jnp.sum(c * c, axis=0, keepdims=True) * (1.0 / model)
        return (c * lax.rsqrt(var + LN_EPSILON) * gain + shift).astype(BF16)

    def column(layer, j, lane):
        return wa_ref[layer, j, :, lane:lane + 1].astype(F32)

    def unpack(layer):
        block = 4 * HEAD_DIM
        row = lax.broadcasted_iota(jnp.int32, (block, block), 0)
        col = lax.broadcasted_iota(jnp.int32, (block, block), 1)
        perm = (col == lax.rem(row, HEAD_DIM) * 4 + row // HEAD_DIM).astype(F32).astype(BF16)
        for h in range(heads):
            mixed = mm(perm, g_ref[layer, h * block:(h + 1) * block, 0:aug]).astype(BF16)
            for j in range(4):
                wa_ref[layer, j, h * HEAD_DIM:(h + 1) * HEAD_DIM, :] = mixed[j * HEAD_DIM:(j + 1) * HEAD_DIM]

    scale = HEAD_DIM ** -0.25
    half = TILE // 2
    eye_k = eye(TILE // 2)

    def norm(layer, t, which):
        gain, shift = column(layer, which, model + 1), column(layer, which + 1, model + 1)
        a_ref[t, 0:model, :] = layer_norm(h_ref[t].astype(F32), gain, shift)

    def project(layer, t):
        a = a_ref[t]
        kt = (mm(wa_ref[layer, 1], a) * scale).astype(BF16)
        q = (mm(wa_ref[layer, 0], a) * scale).astype(BF16)
        for h in range(heads):
            lo = HEAD_DIM * (h % 2)
            q_ref[h, t, lo:lo + HEAD_DIM, :] = q[h * HEAD_DIM:(h + 1) * HEAD_DIM]
        v = mm(wa_ref[layer, 2], a).astype(BF16)
        for h in range(heads):
            v_ref[h, 0:HEAD_DIM, t * TILE:(t + 1) * TILE] = v[h * HEAD_DIM:(h + 1) * HEAD_DIM]
        for b in range(2):
            kn = mm_nt(eye_k, kt[:, b * half:(b + 1) * half]).astype(BF16)
            for p in range(pairs):
                k_ref[p, t * TILE + b * half:t * TILE + (b + 1) * half, :] = kn[:, p * LANES:(p + 1) * LANES]

    s_refs, m_refs = (s0_ref, s1_ref), (m0_ref, m1_ref)

    blocks = [(lo, min(KEY_BLOCK, keys - lo)) for lo in range(0, keys, KEY_BLOCK)]
    steps = [(hh, t) for hh in range(2) for t in range(tiles)]

    def scores(p, j, c, top):
        (hh, t), (lo, size) = steps[j], blocks[c]
        s_ref = s_refs[j % 2]
        s = mm(k_ref[p, lo:lo + size, :], q_ref[2 * p + hh, t])
        whole = size
        if lo + size > frames:
            whole = size - 8
            row = lax.broadcasted_iota(jnp.int32, (8, TILE), 0) + (lo + whole)
            tail = jnp.where(row < frames, s[whole:], -jnp.inf)
            s_ref[lo + whole:lo + size, :] = tail
            top = jnp.maximum(top, tail)
        s_ref[lo:lo + whole, :] = s[0:whole]
        high = jnp.max(s[0:whole].reshape(whole // 8, 8, TILE), axis=0)
        top = high if top is None else jnp.maximum(top, high)
        if c == len(blocks) - 1:
            m_refs[j % 2][...] = jnp.broadcast_to(jnp.max(top, axis=0, keepdims=True), top.shape)
        return top

    def values(p, j, c, total):
        (hh, t), (lo, size) = steps[j], blocks[c]
        h = 2 * p + hh
        s = s_refs[j % 2][lo:lo + size, :].reshape(size // 8, 8, TILE)
        e = jnp.exp(s - m_refs[j % 2][...][None]).reshape(size, TILE).astype(BF16)
        part = mm(v_ref[h, :, lo:lo + size], e)
        total = part if c == 0 else total + part
        if c == len(blocks) - 1:
            inv = 1.0 / total[HEAD_DIM:HEAD_DIM + 1]
            o_ref[t, pl.ds(pl.multiple_of(h * HEAD_DIM, HEAD_DIM), HEAD_DIM), :] = (total[0:HEAD_DIM] * inv).astype(BF16)
        return total

    def attention(events):
        count = len(blocks)

        def body(p, carry):
            total = acc_ref[...]
            for j in range(len(steps)):
                for at, actions in events.items():
                    if j == 0 and actions:
                        pl.when(p == at)(functools.partial(run, actions))
                top = None
                for c in range(count):
                    top = scores(p, j, c, top)
                    back, at = divmod(j * count + c - LAG - count, count)
                    if back < 0:
                        total = values(jnp.maximum(p - 1, 0), back + len(steps), at, total)
                    else:
                        total = values(p, back, at, total)
            acc_ref[...] = total
            return carry

        lax.fori_loop(0, pairs, body, 0)
        total = acc_ref[...]
        for k in range(len(steps) * count - LAG - count, len(steps) * count):
            total = values(pairs - 1, *divmod(k, count), total)

    def unpack_mlp(layer):
        for b in range(hidden // TILE):
            w2 = g_ref[layer, b * TILE:(b + 1) * TILE, 2 * aug:2 * aug + model]
            w2t_ref[:, b * TILE:(b + 1) * TILE] = mm_nt(eye_m, w2).astype(BF16)

    def out_project(layer, t):
        r = h_ref[t].astype(F32) + mm(wa_ref[layer, 3], o_ref[t])
        h_ref[t] = r.astype(BF16)

    def mlp(layer, t):
        c = a_ref[t]
        step = 2 * LANES
        for b in range(hidden // step):
            u = mm(g_ref[layer, b * step:(b + 1) * step, aug:2 * aug], c)
            z_ref[b * step:(b + 1) * step, :] = (0.5 * u * (1.0 + lax.erf(u * (2.0 ** -0.5)))).astype(BF16)
        y = h_ref[t].astype(F32) + (mm(w2t_ref[...], z_ref[...]) + column(layer, 0, model + 2))
        h_ref[t] = y.astype(BF16)

    def out_copy(t):
        rows_out = pl.ds(pl.multiple_of(t * TILE, TILE), TILE)
        return pltpu.make_async_copy(y_ref.at[rows_out, :], out_hbm.at[rows_out, :], out_sem.at[t])

    def write_out(t):
        for b in range(2):
            y = mm_nt(eye_k, h_ref[t, :, b * half:(b + 1) * half]).astype(BF16)
            y_ref[pl.ds(pl.multiple_of(t * TILE + b * half, half), half), :] = y
        out_copy(t).start()

    finish(0)
    unpack(0)
    norm(0, 0, 0)
    for t in range(tiles):
        if t + 1 < tiles:
            norm(0, t + 1, 0)
        project(0, t)

    for layer in range(layers):
        more = layer + 1 < layers
        this, after = 2 * layer + 1, 2 * layer + 2
        events = {0: [], 1: [], pairs - 1: []}
        if layer == 0:
            events[0] += plan.step(this, 2)
        elif more:
            events[0] += plan.step(after, 1)
        if more:
            events[1] += plan.step(after, 2) + plan.step(after + 1, 1)
        events[pairs - 1] += plan.hand_over(this, everything=True)
        attention(events)
        finish(this)
        if more:
            run(plan.hand_over(after, everything=True))
        out_project(layer, 0)
        out_project(layer, 1)
        norm(layer, 0, 2)
        out_project(layer, 2)
        unpack_mlp(layer)
        norm(layer, 1, 2)
        mlp(layer, 0)
        if more:
            run(plan.step(after + 1, 2))
            finish(after)
            unpack(layer + 1)
        else:
            write_out(0)
        norm(layer, 2, 2)
        for t in range(1, tiles):
            mlp(layer, t)
            if more:
                norm(layer + 1, t - 1, 0)
            else:
                write_out(t)
        if more:
            for t in range(tiles):
                if t == 1:
                    norm(layer + 1, tiles - 1, 0)
                project(layer + 1, t)

    for t in range(tiles):
        out_copy(t).wait()

    for piece in range(len(pieces)):
        for m in range(len(MESSAGES)):
            relay(piece, m).wait_send()
        for b in handed(piece):
            hand(piece, b).wait_send()


def solution(mesh):
    n = mesh.shape["dp"]

    def body(audio_x, attn_w, fc1_w, fc2_w, vec_d, b1_vec):
        layers, four, model, cols = attn_w.shape
        hidden_cols = fc1_w.shape[2]
        batch, frames, _ = audio_x.shape
        hidden = hidden_cols * n
        aug = model + LANES
        rows = four * cols
        attn = jnp.transpose(attn_w, (0, 3, 1, 2))
        fc1 = jnp.transpose(fc1_w, (0, 2, 1))

        tiles = -(-frames // TILE)
        padded = tiles * TILE
        keys = -(-frames // 16) * 16
        heads = model // HEAD_DIM
        pieces = 2 * layers
        out = pl.pallas_call(
            functools.partial(kernel, n),
            out_shape=jax.ShapeDtypeStruct((padded, model), audio_x.dtype),
            in_specs=[pl.BlockSpec(memory_space=pl.ANY)] * 6,
            out_specs=pl.BlockSpec(memory_space=pl.ANY),
            scratch_shapes=[
                pltpu.VMEM(attn.shape, BF16),
                pltpu.VMEM(fc1.shape, BF16),
                pltpu.VMEM(fc2_w.shape, BF16),
                pltpu.VMEM(vec_d.shape, BF16),
                pltpu.VMEM(b1_vec.shape, BF16),
                pltpu.VMEM((layers, rows, 2 * aug + model), BF16),
                pltpu.VMEM((rows, model), F32),
                pltpu.VMEM((layers, n * rows, 2 * aug + model), BF16),
                pltpu.VMEM((layers, four, model, aug), BF16),
                pltpu.VMEM((model, hidden), BF16),
                pltpu.VMEM((frames, model), BF16),
                pltpu.VMEM((padded, model), BF16),
                pltpu.VMEM((tiles, model, TILE), BF16),
                pltpu.VMEM((tiles, aug, TILE), BF16),
                pltpu.VMEM((heads, tiles, LANES, TILE), BF16),
                pltpu.VMEM((heads // 2, padded, LANES), BF16),
                pltpu.VMEM((heads, HEAD_DIM + 16, padded), BF16),
                pltpu.VMEM((tiles, aug, TILE), BF16),
                pltpu.VMEM((hidden, TILE), BF16),
                pltpu.VMEM((keys, TILE), F32),
                pltpu.VMEM((keys, TILE), F32),
                pltpu.VMEM((8, TILE), F32),
                pltpu.VMEM((8, TILE), F32),
                pltpu.VMEM((HEAD_DIM + 16, TILE), F32),
                pltpu.SemaphoreType.DMA((6,)),
                pltpu.SemaphoreType.DMA((tiles,)),
                pltpu.SemaphoreType.DMA((pieces, len(MESSAGES))),
                pltpu.SemaphoreType.DMA((pieces, len(MESSAGES))),
                pltpu.SemaphoreType.DMA((pieces, len(BLOCKS) + 1)),
                pltpu.SemaphoreType.DMA((pieces, len(BLOCKS) + 1)),
            ],
            compiler_params=pltpu.CompilerParams(
                collective_id=0, has_side_effects=True, vmem_limit_bytes=60 * 1024 * 1024),
        )(audio_x, attn, fc1, fc2_w, vec_d, b1_vec)
        return out[None, :frames]

    return jax.shard_map(
        body, mesh=mesh,
        in_specs=(P(('rep', 'dp')), P(None, None, None, 'dp'), P(None, None, 'dp'), P(None, 'dp', None), P(None, None, 'dp'), P(None, 'dp')),
        out_specs=P(('rep', 'dp')), check_vma=False)
```

```python
import functools

import jax
import jax.numpy as jnp
from jax import lax
from jax.experimental import pallas as pl
from jax.experimental.pallas import tpu as pltpu
from jax.sharding import PartitionSpec as P

HEAD_DIM = 64
LN_EPSILON = 1e-5
LANES = 128
TILE = 512
KEY_BLOCK = 256
LAG = 2
F32, BF16 = jnp.float32, jnp.bfloat16
NT = (((1,), (1,)), ((), ()))


def mm(a, b):
    return jnp.dot(a, b, preferred_element_type=F32)


def mm_nt(a, b):
    return lax.dot_general(a, b, NT, preferred_element_type=F32)


def eye(n):
    row = lax.broadcasted_iota(jnp.int32, (n, n), 0)
    col = lax.broadcasted_iota(jnp.int32, (n, n), 1)
    return (row == col).astype(F32).astype(BF16)


RING = 4


def relay_plan():
    messages, complete = [], {}

    def add(*message):
        messages.append(message)
        return len(messages) - 1

    def at(a, b):
        return a % RING, b % RING

    both = (1, -1)
    axes = [(1, 0), (-1, 0), (0, 1), (0, -1)]
    corners = [(a, b) for a in both for b in both]
    own = {to: add(1, (0, 1), at(0, 0), to, ()) for to in axes + corners}
    for (a, b), m in own.items():
        complete[at(-a, -b)] = (m,)
    for part, s in enumerate(both):
        for r in (0, 1, -1):
            m = add(2, (part, 2), at(-s, -r), (s, 0), (own[s, r],))
            complete[at(2, -r)] = complete.get(at(2, -r), ()) + (m,)
            m = add(2, (part, 2), at(-r, -s), (0, s), (own[r, s],))
            complete[at(-r, 2)] = complete.get(at(-r, 2), ()) + (m,)
    for part, (a, b) in enumerate(corners):
        m = add(2, (part, 4), at(-a, -b), (a, b), (own[a, b],))
        complete[at(2, 2)] = complete.get(at(2, 2), ()) + (m,)
    return messages, complete


MESSAGES, COMPLETE = relay_plan()
BLOCKS = list(COMPLETE)


class Planner:
    def __init__(self):
        self.arrived, self.passed = set(), set()

    def step(self, piece, step):
        actions = []
        for m, message in enumerate(MESSAGES):
            if message[0] == step:
                actions += self.need(piece, message[-1])
                actions.append(("start", piece, m))
        if step == 1 and piece == 0:
            actions.append(("pass", piece, len(BLOCKS)))
        return actions + self.hand_over(piece)

    def need(self, piece, deps):
        actions = [("wait", piece, m) for m in deps if (piece, m) not in self.arrived]
        self.arrived.update((piece, m) for m in deps)
        return actions

    def hand_over(self, piece, everything=False):
        if piece:
            if not everything or (piece, "all") in self.passed:
                return []
            self.passed.add((piece, "all"))
            return self.need(piece, range(len(MESSAGES))) + [("pass", piece, len(BLOCKS))]
        actions = []
        for b, block in enumerate(BLOCKS):
            if (piece, b) in self.passed:
                continue
            if everything:
                actions += self.need(piece, COMPLETE[block])
            if all((piece, m) in self.arrived for m in COMPLETE[block]):
                actions.append(("pass", piece, b))
                self.passed.add((piece, b))
        if everything:
            actions += self.need(piece, range(len(MESSAGES)))
        return actions


def kernel(n, x_hbm, attn_hbm, fc1_hbm, fc2_hbm, vec_hbm, b1_hbm, out_hbm, attn_ref, fc1_ref, fc2_ref, vec_ref, b1_ref, w_ref, row_ref, g_ref, wa_ref, w2t_ref, x_ref, y_ref, h_ref, a_ref,
           q_ref, k_ref, v_ref, o_ref, z_ref, s0_ref, s1_ref, m0_ref, m1_ref, acc_ref, x_sem, out_sem, send_sem, recv_sem, fsend_sem, frecv_sem):
    layers, rows, width = w_ref.shape
    _, frames, model = x_hbm.shape
    aug = wa_ref.shape[3]
    heads = model // HEAD_DIM
    pairs = heads // 2
    hidden = z_ref.shape[0]
    tiles = h_ref.shape[0]
    keys = s0_ref.shape[0]

    me = lax.axis_index("dp")
    core = lax.rem(me, 2)
    chip = me // 2
    chip_x, chip_y = lax.rem(chip, RING), chip // RING

    @functools.cache
    def device(offset):
        x = lax.rem(chip_x + offset[0] + RING, RING)
        y = lax.rem(chip_y + offset[1] + RING, RING)
        return 2 * (y * RING + x) + core

    partner = me + 1 - 2 * core
    neighbour = {to: device((to[0] % RING, to[1] % RING)) for step, _, _, to, _ in MESSAGES if step == 1}
    for offset in BLOCKS + [(0, 0)]:
        device(offset)

    barrier = pltpu.get_barrier_semaphore()
    for dev in [*neighbour.values(), partner]:
        pl.semaphore_signal(barrier, inc=1, device_id={"dp": dev})

    fetches = [pltpu.make_async_copy(src, dst, x_sem.at[i]) for i, (src, dst) in enumerate([
        (attn_hbm, attn_ref), (vec_hbm, vec_ref), (fc1_hbm, fc1_ref), (fc2_hbm, fc2_ref), (b1_hbm, b1_ref), (x_hbm.at[0], x_ref)])]
    for fetch in fetches:
        fetch.start()
    fetch_x = fetches.pop()

    ones_row = (lax.broadcasted_iota(jnp.int32, (aug - model, TILE), 0) == 0).astype(F32).astype(BF16)
    for t in range(tiles):
        a_ref[t, model:, :] = ones_row
        o_ref[t, model:, :] = ones_row
    for fetch in fetches:
        fetch.wait()

    def pick(layer, want):
        row = lax.broadcasted_iota(jnp.int32, (rows, vec_ref.shape[1]), 0)
        col = lax.broadcasted_iota(jnp.int32, (rows, vec_ref.shape[1]), 1)
        sel = jnp.zeros(row.shape, F32)
        for j, r in enumerate(want):
            if r is not None:
                sel = jnp.where((lax.rem(row, 4) == j) & (col == r), 1.0, sel)
        spread = mm(sel, vec_ref[layer].astype(F32))
        row = lax.broadcasted_iota(jnp.int32, spread.shape, 0)
        col = lax.broadcasted_iota(jnp.int32, spread.shape, 1)
        return jnp.sum(jnp.where(row // 4 == col, spread, 0.0), axis=1, keepdims=True)

    lane = lax.broadcasted_iota(jnp.int32, (rows, LANES), 1)
    for layer in range(layers):
        for c in range(rows // 4):
            row_ref[4 * c:4 * c + 4, :] = attn_ref[layer, c].astype(F32)
        w_ref[layer, :, 0:model] = row_ref[...].astype(BF16)
        entry = [pick(layer, want) for want in ((0, None, 1, 2), (4, 5, 6, 7), (3, None, None, None))]
        extra = jnp.where(lane == 0, entry[0], jnp.where(lane == 1, entry[1], jnp.where(lane == 2, entry[2], 0.0)))
        w_ref[layer, :, model:aug] = extra.astype(BF16)
        w_ref[layer, :, aug:aug + model] = fc1_ref[layer]
        row = lax.broadcasted_iota(jnp.int32, (rows, rows), 0)
        col = lax.broadcasted_iota(jnp.int32, (rows, rows), 1)
        b1 = jnp.sum(jnp.where(row == col, b1_ref[layer:layer + 1, :].astype(F32), 0.0), axis=1, keepdims=True)
        w_ref[layer, :, aug + model:2 * aug] = jnp.where(lane == 0, b1, 0.0).astype(BF16)
        w_ref[layer, :, 2 * aug:width] = fc2_ref[layer]

    own = pl.ds(pl.multiple_of(me * rows, 16), rows)
    for layer in range(layers):
        g_ref[layer, own, :] = w_ref[layer]
    pl.semaphore_wait(barrier, len(neighbour) + 1)

    pieces = [piece for layer in range(layers) for piece in ((layer, 0, aug), (layer, aug, width - aug))]

    def lanes_of(piece, part, parts):
        _, lo, size = pieces[piece]
        units = size // LANES
        first, last = -(-units * part // parts), -(-units * (part + 1) // parts)
        return pl.ds(lo + first * LANES, (last - first) * LANES)

    def slot(piece, dev, lanes):
        return g_ref.at[pieces[piece][0], pl.ds(pl.multiple_of(dev * rows, 16), rows), lanes]

    def relay(piece, m):
        step, part, offset, to, _ = MESSAGES[m]
        lanes = lanes_of(piece, *part)
        dst = slot(piece, device(offset), lanes)
        src = w_ref.at[pieces[piece][0], :, lanes] if step == 1 else dst
        return pltpu.make_async_remote_copy(
            src_ref=src, dst_ref=dst, send_sem=send_sem.at[piece, m], recv_sem=recv_sem.at[piece, m],
            device_id={"dp": neighbour[to]})

    def hand(piece, b):
        lanes = lanes_of(piece, 0, 1)
        if piece:
            src = dst = g_ref.reshape(layers, n // 2, 2, rows, width).at[pieces[piece][0], :, core, :, lanes]
        elif b == len(BLOCKS):
            src, dst = w_ref.at[pieces[piece][0], :, lanes], slot(piece, me, lanes)
        else:
            src = dst = slot(piece, device(BLOCKS[b]), lanes)
        return pltpu.make_async_remote_copy(
            src_ref=src, dst_ref=dst, send_sem=fsend_sem.at[piece, b], recv_sem=frecv_sem.at[piece, b],
            device_id={"dp": partner})

    def run(actions):
        for kind, piece, index in actions:
            if kind == "start":
                relay(piece, index).start()
            elif kind == "wait":
                relay(piece, index).wait_recv()
            else:
                hand(piece, index).start()

    def finish(piece):
        run(plan.hand_over(piece, everything=True))
        for b in handed(piece):
            hand(piece, b).wait_recv()

    def handed(piece):
        return range(len(BLOCKS) + 1) if piece == 0 else [len(BLOCKS)]

    plan = Planner()
    run(plan.step(0, 1))

    zero_half = jnp.zeros((HEAD_DIM, TILE), BF16)
    for h in range(heads):
        other = HEAD_DIM * (1 - h % 2)
        for t in range(tiles):
            q_ref[h, t, other:other + HEAD_DIM, :] = zero_half
        extra = v_ref.shape[1] - HEAD_DIM
        v_ref[h, HEAD_DIM:, :] = (lax.broadcasted_iota(jnp.int32, (extra, v_ref.shape[2]), 0) == 0).astype(F32).astype(BF16)

    eye_m = eye(model)
    h_ref[tiles - 1, :, :] = jnp.zeros((model, TILE), BF16)
    fetch_x.wait()
    for t in range(tiles):
        size = min(TILE, frames - t * TILE)
        h_ref[t, :, 0:size] = mm_nt(eye_m, x_ref[t * TILE:t * TILE + size, :]).astype(BF16)

    run(plan.step(0, 2))
    run(plan.step(1, 1))
    if layers > 1:
        run(plan.step(2, 1))

    def layer_norm(z, gain, shift):
        mean = jnp.sum(z, axis=0, keepdims=True) * (1.0 / model)
        c = z - mean
        var = jnp.sum(c * c, axis=0, keepdims=True) * (1.0 / model)
        return (c * lax.rsqrt(var + LN_EPSILON) * gain + shift).astype(BF16)

    def column(layer, j, lane):
        return wa_ref[layer, j, :, lane:lane + 1].astype(F32)

    def unpack(layer):
        block = 4 * HEAD_DIM
        row = lax.broadcasted_iota(jnp.int32, (block, block), 0)
        col = lax.broadcasted_iota(jnp.int32, (block, block), 1)
        perm = (col == lax.rem(row, HEAD_DIM) * 4 + row // HEAD_DIM).astype(F32).astype(BF16)
        for h in range(heads):
            mixed = mm(perm, g_ref[layer, h * block:(h + 1) * block, 0:aug]).astype(BF16)
            for j in range(4):
                wa_ref[layer, j, h * HEAD_DIM:(h + 1) * HEAD_DIM, :] = mixed[j * HEAD_DIM:(j + 1) * HEAD_DIM]

    scale = HEAD_DIM ** -0.25
    half = TILE // 2
    eye_k = eye(TILE // 2)

    def norm(layer, t, which):
        gain, shift = column(layer, which, model + 1), column(layer, which + 1, model + 1)
        for lo in range(0, TILE, LANES):
            a_ref[t, 0:model, lo:lo + LANES] = layer_norm(h_ref[t, :, lo:lo + LANES].astype(F32), gain, shift)

    def project(layer, t):
        a = a_ref[t]
        kt = (mm(wa_ref[layer, 1], a) * scale).astype(BF16)
        q = (mm(wa_ref[layer, 0], a) * scale).astype(BF16)
        for h in range(heads):
            lo = HEAD_DIM * (h % 2)
            q_ref[h, t, lo:lo + HEAD_DIM, :] = q[h * HEAD_DIM:(h + 1) * HEAD_DIM]
        v = mm(wa_ref[layer, 2], a).astype(BF16)
        for h in range(heads):
            v_ref[h, 0:HEAD_DIM, t * TILE:(t + 1) * TILE] = v[h * HEAD_DIM:(h + 1) * HEAD_DIM]
        for b in range(2):
            kn = mm_nt(eye_k, kt[:, b * half:(b + 1) * half]).astype(BF16)
            for p in range(pairs):
                k_ref[p, t * TILE + b * half:t * TILE + (b + 1) * half, :] = kn[:, p * LANES:(p + 1) * LANES]

    s_refs, m_refs = (s0_ref, s1_ref), (m0_ref, m1_ref)

    blocks = [(lo, min(KEY_BLOCK, keys - lo)) for lo in range(0, keys, KEY_BLOCK)]
    steps = [(hh, t) for hh in range(2) for t in range(tiles)]

    def scores(p, j, c, top):
        (hh, t), (lo, size) = steps[j], blocks[c]
        s_ref = s_refs[j % 2]
        s = mm(k_ref[p, lo:lo + size, :], q_ref[2 * p + hh, t])
        whole = size
        if lo + size > frames:
            whole = size - 8
            row = lax.broadcasted_iota(jnp.int32, (8, TILE), 0) + (lo + whole)
            tail = jnp.where(row < frames, s[whole:], -jnp.inf)
            s_ref[lo + whole:lo + size, :] = tail
            top = jnp.maximum(top, tail)
        s_ref[lo:lo + whole, :] = s[0:whole]
        high = jnp.max(s[0:whole].reshape(whole // 8, 8, TILE), axis=0)
        top = high if top is None else jnp.maximum(top, high)
        if c == len(blocks) - 1:
            m_refs[j % 2][...] = jnp.broadcast_to(jnp.max(top, axis=0, keepdims=True), top.shape)
        return top

    def values(p, j, c, total):
        (hh, t), (lo, size) = steps[j], blocks[c]
        h = 2 * p + hh
        s = s_refs[j % 2][lo:lo + size, :].reshape(size // 8, 8, TILE)
        e = jnp.exp(s - m_refs[j % 2][...][None]).reshape(size, TILE).astype(BF16)
        part = mm(v_ref[h, :, lo:lo + size], e)
        total = part if c == 0 else total + part
        if c == len(blocks) - 1:
            inv = 1.0 / total[HEAD_DIM:HEAD_DIM + 1]
            o_ref[t, pl.ds(pl.multiple_of(h * HEAD_DIM, HEAD_DIM), HEAD_DIM), :] = (total[0:HEAD_DIM] * inv).astype(BF16)
        return total

    def attention(events, before_tail, fillers):
        count = len(blocks)

        def body(p, carry):
            total = acc_ref[...]
            for j in range(len(steps)):
                for at, actions in events.items():
                    if j == 0 and actions:
                        pl.when(p == at)(functools.partial(run, actions))
                top = None
                for c in range(count):
                    top = scores(p, j, c, top)
                    back, at = divmod(j * count + c - LAG - count, count)
                    if back < 0:
                        total = values(jnp.maximum(p - 1, 0), back + len(steps), at, total)
                    else:
                        total = values(p, back, at, total)
            acc_ref[...] = total
            return carry

        lax.fori_loop(0, pairs, body, 0)
        before_tail()
        total = acc_ref[...]
        for k in range(len(steps) * count - LAG - count, len(steps) * count):
            total = values(pairs - 1, *divmod(k, count), total)
            if fillers:
                fillers.pop(0)()

    def unpack_mlp(layer, b):
        w2 = g_ref[layer, b * TILE:(b + 1) * TILE, 2 * aug:2 * aug + model]
        w2t_ref[:, b * TILE:(b + 1) * TILE] = mm_nt(eye_m, w2).astype(BF16)

    def out_project(layer, t):
        r = h_ref[t].astype(F32) + mm(wa_ref[layer, 3], o_ref[t])
        h_ref[t] = r.astype(BF16)

    def mlp(layer, t):
        c = a_ref[t]
        step = 2 * LANES
        for b in range(hidden // step):
            u = mm(g_ref[layer, b * step:(b + 1) * step, aug:2 * aug], c)
            z_ref[b * step:(b + 1) * step, :] = (0.5 * u * (1.0 + lax.erf(u * (2.0 ** -0.5)))).astype(BF16)
        y = h_ref[t].astype(F32) + (mm(w2t_ref[...], z_ref[...]) + column(layer, 0, model + 2))
        h_ref[t] = y.astype(BF16)

    def out_copy(t):
        rows_out = pl.ds(pl.multiple_of(t * TILE, TILE), TILE)
        return pltpu.make_async_copy(y_ref.at[rows_out, :], out_hbm.at[rows_out, :], out_sem.at[t])

    def write_out(t):
        for b in range(2):
            y = mm_nt(eye_k, h_ref[t, :, b * half:(b + 1) * half]).astype(BF16)
            y_ref[pl.ds(pl.multiple_of(t * TILE + b * half, half), half), :] = y
        out_copy(t).start()

    finish(0)
    unpack(0)
    norm(0, 0, 0)
    for t in range(tiles):
        if t + 1 < tiles:
            norm(0, t + 1, 0)
        project(0, t)

    for layer in range(layers):
        more = layer + 1 < layers
        this, after = 2 * layer + 1, 2 * layer + 2
        events = {0: [], 1: [], pairs - 1: []}
        if layer == 0:
            events[0] += plan.step(this, 2)
        elif more:
            events[0] += plan.step(after, 1)
        if more:
            events[1] += plan.step(after, 2) + plan.step(after + 1, 1)
        events[pairs - 1] += plan.hand_over(this, everything=True)
        fillers = [functools.partial(unpack_mlp, layer, b) for b in range(hidden // TILE)]
        fillers.insert(2, functools.partial(out_project, layer, 0))
        fillers += [functools.partial(out_project, layer, 1), functools.partial(norm, layer, 0, 2)]
        attention(events, functools.partial(finish, this), fillers)
        if more:
            run(plan.hand_over(after, everything=True))
        out_project(layer, 2)
        norm(layer, 1, 2)
        mlp(layer, 0)
        if more:
            run(plan.step(after + 1, 2))
            finish(after)
            unpack(layer + 1)
        else:
            write_out(0)
        norm(layer, 2, 2)
        for t in range(1, tiles):
            mlp(layer, t)
            if more:
                norm(layer + 1, t - 1, 0)
            else:
                write_out(t)
        if more:
            for t in range(tiles):
                if t == 1:
                    norm(layer + 1, tiles - 1, 0)
                project(layer + 1, t)

    for piece in range(len(pieces)):
        for m in range(len(MESSAGES)):
            relay(piece, m).wait_send()
        for b in handed(piece):
            hand(piece, b).wait_send()

    for t in range(tiles):
        out_copy(t).wait()


def solution(mesh):
    n = mesh.shape["dp"]

    def body(audio_x, attn_w, fc1_w, fc2_w, vec_d, b1_vec):
        layers, four, model, cols = attn_w.shape
        hidden_cols = fc1_w.shape[2]
        batch, frames, _ = audio_x.shape
        hidden = hidden_cols * n
        aug = model + LANES
        rows = four * cols
        attn = jnp.transpose(attn_w, (0, 3, 1, 2))
        fc1 = jnp.transpose(fc1_w, (0, 2, 1))

        tiles = -(-frames // TILE)
        padded = tiles * TILE
        keys = -(-frames // 16) * 16
        heads = model // HEAD_DIM
        pieces = 2 * layers
        out = pl.pallas_call(
            functools.partial(kernel, n),
            out_shape=jax.ShapeDtypeStruct((padded, model), audio_x.dtype),
            in_specs=[pl.BlockSpec(memory_space=pl.ANY)] * 6,
            out_specs=pl.BlockSpec(memory_space=pl.ANY),
            scratch_shapes=[
                pltpu.VMEM(attn.shape, BF16),
                pltpu.VMEM(fc1.shape, BF16),
                pltpu.VMEM(fc2_w.shape, BF16),
                pltpu.VMEM(vec_d.shape, BF16),
                pltpu.VMEM(b1_vec.shape, BF16),
                pltpu.VMEM((layers, rows, 2 * aug + model), BF16),
                pltpu.VMEM((rows, model), F32),
                pltpu.VMEM((layers, n * rows, 2 * aug + model), BF16),
                pltpu.VMEM((layers, four, model, aug), BF16),
                pltpu.VMEM((model, hidden), BF16),
                pltpu.VMEM((frames, model), BF16),
                pltpu.VMEM((padded, model), BF16),
                pltpu.VMEM((tiles, model, TILE), BF16),
                pltpu.VMEM((tiles, aug, TILE), BF16),
                pltpu.VMEM((heads, tiles, LANES, TILE), BF16),
                pltpu.VMEM((heads // 2, padded, LANES), BF16),
                pltpu.VMEM((heads, HEAD_DIM + 16, padded), BF16),
                pltpu.VMEM((tiles, aug, TILE), BF16),
                pltpu.VMEM((hidden, TILE), BF16),
                pltpu.VMEM((keys, TILE), F32),
                pltpu.VMEM((keys, TILE), F32),
                pltpu.VMEM((8, TILE), F32),
                pltpu.VMEM((8, TILE), F32),
                pltpu.VMEM((HEAD_DIM + 16, TILE), F32),
                pltpu.SemaphoreType.DMA((6,)),
                pltpu.SemaphoreType.DMA((tiles,)),
                pltpu.SemaphoreType.DMA((pieces, len(MESSAGES))),
                pltpu.SemaphoreType.DMA((pieces, len(MESSAGES))),
                pltpu.SemaphoreType.DMA((pieces, len(BLOCKS) + 1)),
                pltpu.SemaphoreType.DMA((pieces, len(BLOCKS) + 1)),
            ],
            compiler_params=pltpu.CompilerParams(
                collective_id=0, has_side_effects=True, vmem_limit_bytes=60 * 1024 * 1024),
        )(audio_x, attn, fc1, fc2_w, vec_d, b1_vec)
        return out[None, :frames]

    return jax.shard_map(
        body, mesh=mesh,
        in_specs=(P(('rep', 'dp')), P(None, None, None, 'dp'), P(None, None, 'dp'), P(None, 'dp', None), P(None, None, 'dp'), P(None, 'dp')),
        out_specs=P(('rep', 'dp')), check_vma=False)
```

```python
import functools

import jax
import jax.numpy as jnp
from jax import lax
from jax.experimental import pallas as pl
from jax.experimental.pallas import tpu as pltpu
from jax.sharding import PartitionSpec as P

HEAD_DIM = 64
LN_EPSILON = 1e-5
LANES = 128
TILE = 512
KEY_BLOCK = 256
LAG = 2
F32, BF16 = jnp.float32, jnp.bfloat16
NT = (((1,), (1,)), ((), ()))


def mm(a, b):
    return jnp.dot(a, b, preferred_element_type=F32)


def mm_nt(a, b):
    return lax.dot_general(a, b, NT, preferred_element_type=F32)


def eye(n):
    row = lax.broadcasted_iota(jnp.int32, (n, n), 0)
    col = lax.broadcasted_iota(jnp.int32, (n, n), 1)
    return (row == col).astype(F32).astype(BF16)


RING = 4


def relay_plan():
    messages, complete = [], {}

    def add(*message):
        messages.append(message)
        return len(messages) - 1

    def at(a, b):
        return a % RING, b % RING

    both = (1, -1)
    axes = [(1, 0), (-1, 0), (0, 1), (0, -1)]
    corners = [(a, b) for a in both for b in both]
    own = {to: add(1, (0, 1), at(0, 0), to, ()) for to in corners + axes}
    for (a, b), m in own.items():
        complete[at(-a, -b)] = (m,)
    for part, (a, b) in enumerate(corners):
        m = add(2, (part, 4), at(-a, -b), (a, b), (own[a, b],))
        complete[at(2, 2)] = complete.get(at(2, 2), ()) + (m,)
    for r in (1, -1, 0):
        for part, s in enumerate(both):
            m = add(2, (part, 2), at(-s, -r), (s, 0), (own[s, r],))
            complete[at(2, -r)] = complete.get(at(2, -r), ()) + (m,)
            m = add(2, (part, 2), at(-r, -s), (0, s), (own[r, s],))
            complete[at(-r, 2)] = complete.get(at(-r, 2), ()) + (m,)
    return messages, complete


MESSAGES, COMPLETE = relay_plan()
BLOCKS = list(COMPLETE)


class Planner:
    def __init__(self):
        self.arrived, self.passed = set(), set()

    def step(self, piece, step):
        actions = []
        for m, message in enumerate(MESSAGES):
            if message[0] == step:
                actions += self.need(piece, message[-1])
                actions.append(("start", piece, m))
        if step == 1 and piece == 0:
            actions.append(("pass", piece, len(BLOCKS)))
        return actions + self.hand_over(piece)

    def need(self, piece, deps):
        actions = [("wait", piece, m) for m in deps if (piece, m) not in self.arrived]
        self.arrived.update((piece, m) for m in deps)
        return actions

    def hand_over(self, piece, everything=False):
        if piece:
            if not everything or (piece, "all") in self.passed:
                return []
            self.passed.add((piece, "all"))
            return self.need(piece, range(len(MESSAGES))) + [("pass", piece, len(BLOCKS))]
        actions = []
        for b, block in enumerate(BLOCKS):
            if (piece, b) in self.passed:
                continue
            if everything:
                actions += self.need(piece, COMPLETE[block])
            if all((piece, m) in self.arrived for m in COMPLETE[block]):
                actions.append(("pass", piece, b))
                self.passed.add((piece, b))
        if everything:
            actions += self.need(piece, range(len(MESSAGES)))
        return actions


def kernel(n, x_hbm, attn_hbm, fc1_hbm, fc2_hbm, vec_hbm, b1_hbm, out_hbm, attn_ref, fc1_ref, fc2_ref, vec_ref, b1_ref, w_ref, row_ref, g_ref, wa_ref, w2t_ref, x_ref, y_ref, xhat_ref, h_ref, a_ref,
           q_ref, k_ref, v_ref, o_ref, z_ref, s0_ref, s1_ref, m0_ref, m1_ref, acc_ref, x_sem, out_sem, send_sem, recv_sem, fsend_sem, frecv_sem):
    layers, rows, width = w_ref.shape
    _, frames, model = x_hbm.shape
    aug = wa_ref.shape[3]
    heads = model // HEAD_DIM
    pairs = heads // 2
    hidden = z_ref.shape[0]
    tiles = h_ref.shape[0]
    keys = s0_ref.shape[0]

    me = lax.axis_index("dp")
    core = lax.rem(me, 2)
    chip = me // 2
    chip_x, chip_y = lax.rem(chip, RING), chip // RING

    @functools.cache
    def device(offset):
        x = lax.rem(chip_x + offset[0] + RING, RING)
        y = lax.rem(chip_y + offset[1] + RING, RING)
        return 2 * (y * RING + x) + core

    partner = me + 1 - 2 * core
    neighbour = {to: device((to[0] % RING, to[1] % RING)) for step, _, _, to, _ in MESSAGES if step == 1}
    for offset in BLOCKS + [(0, 0)]:
        device(offset)

    barrier = pltpu.get_barrier_semaphore()
    for dev in [*neighbour.values(), partner]:
        pl.semaphore_signal(barrier, inc=1, device_id={"dp": dev})

    fetches = [pltpu.make_async_copy(src, dst, x_sem.at[i]) for i, (src, dst) in enumerate([
        (attn_hbm, attn_ref), (vec_hbm, vec_ref), (fc1_hbm, fc1_ref), (fc2_hbm, fc2_ref), (b1_hbm, b1_ref), (x_hbm.at[0], x_ref)])]
    for fetch in fetches:
        fetch.start()
    fetch_x = fetches.pop()

    ones_row = (lax.broadcasted_iota(jnp.int32, (aug - model, TILE), 0) == 0).astype(F32).astype(BF16)
    for t in range(tiles):
        a_ref[t, model:, :] = ones_row
        o_ref[t, model:, :] = ones_row
    for fetch in fetches:
        fetch.wait()

    def pick(layer, want):
        row = lax.broadcasted_iota(jnp.int32, (rows, vec_ref.shape[1]), 0)
        col = lax.broadcasted_iota(jnp.int32, (rows, vec_ref.shape[1]), 1)
        sel = jnp.zeros(row.shape, F32)
        for j, r in enumerate(want):
            if r is not None:
                sel = jnp.where((lax.rem(row, 4) == j) & (col == r), 1.0, sel)
        spread = mm(sel, vec_ref[layer].astype(F32))
        row = lax.broadcasted_iota(jnp.int32, spread.shape, 0)
        col = lax.broadcasted_iota(jnp.int32, spread.shape, 1)
        return jnp.sum(jnp.where(row // 4 == col, spread, 0.0), axis=1, keepdims=True)

    lane = lax.broadcasted_iota(jnp.int32, (rows, LANES), 1)
    for layer in range(layers):
        for c in range(rows // 4):
            row_ref[4 * c:4 * c + 4, :] = attn_ref[layer, c].astype(F32)
        w_ref[layer, :, 0:model] = row_ref[...].astype(BF16)
        entry = [pick(layer, want) for want in ((0, None, 1, 2), (4, 5, 6, 7), (3, None, None, None))]
        extra = jnp.where(lane == 0, entry[0], jnp.where(lane == 1, entry[1], jnp.where(lane == 2, entry[2], 0.0)))
        w_ref[layer, :, model:aug] = extra.astype(BF16)
        w_ref[layer, :, aug:aug + model] = fc1_ref[layer]
        row = lax.broadcasted_iota(jnp.int32, (rows, rows), 0)
        col = lax.broadcasted_iota(jnp.int32, (rows, rows), 1)
        b1 = jnp.sum(jnp.where(row == col, b1_ref[layer:layer + 1, :].astype(F32), 0.0), axis=1, keepdims=True)
        w_ref[layer, :, aug + model:2 * aug] = jnp.where(lane == 0, b1, 0.0).astype(BF16)
        w_ref[layer, :, 2 * aug:width] = fc2_ref[layer]

    own = pl.ds(pl.multiple_of(me * rows, 16), rows)
    for layer in range(layers):
        g_ref[layer, own, :] = w_ref[layer]
    pl.semaphore_wait(barrier, len(neighbour) + 1)

    pieces = [piece for layer in range(layers) for piece in ((layer, 0, aug), (layer, aug, width - aug))]

    def lanes_of(piece, part, parts):
        _, lo, size = pieces[piece]
        units = size // LANES
        first, last = -(-units * part // parts), -(-units * (part + 1) // parts)
        return pl.ds(lo + first * LANES, (last - first) * LANES)

    def slot(piece, dev, lanes):
        return g_ref.at[pieces[piece][0], pl.ds(pl.multiple_of(dev * rows, 16), rows), lanes]

    def relay(piece, m):
        step, part, offset, to, _ = MESSAGES[m]
        lanes = lanes_of(piece, *part)
        dst = slot(piece, device(offset), lanes)
        src = w_ref.at[pieces[piece][0], :, lanes] if step == 1 else dst
        return pltpu.make_async_remote_copy(
            src_ref=src, dst_ref=dst, send_sem=send_sem.at[piece, m], recv_sem=recv_sem.at[piece, m],
            device_id={"dp": neighbour[to]})

    def hand(piece, b):
        lanes = lanes_of(piece, 0, 1)
        if piece:
            src = dst = g_ref.reshape(layers, n // 2, 2, rows, width).at[pieces[piece][0], :, core, :, lanes]
        elif b == len(BLOCKS):
            src, dst = w_ref.at[pieces[piece][0], :, lanes], slot(piece, me, lanes)
        else:
            src = dst = slot(piece, device(BLOCKS[b]), lanes)
        return pltpu.make_async_remote_copy(
            src_ref=src, dst_ref=dst, send_sem=fsend_sem.at[piece, b], recv_sem=frecv_sem.at[piece, b],
            device_id={"dp": partner})

    def run(actions):
        for kind, piece, index in actions:
            if kind == "start":
                relay(piece, index).start()
            elif kind == "wait":
                relay(piece, index).wait_recv()
            else:
                hand(piece, index).start()

    def finish(piece):
        run(plan.hand_over(piece, everything=True))
        for b in handed(piece):
            hand(piece, b).wait_recv()

    def handed(piece):
        return range(len(BLOCKS) + 1) if piece == 0 else [len(BLOCKS)]

    plan = Planner()
    run(plan.step(0, 1))

    zero_half = jnp.zeros((HEAD_DIM, TILE), BF16)
    for h in range(heads):
        other = HEAD_DIM * (1 - h % 2)
        for t in range(tiles):
            q_ref[h, t, other:other + HEAD_DIM, :] = zero_half
        extra = v_ref.shape[1] - HEAD_DIM
        v_ref[h, HEAD_DIM:, :] = (lax.broadcasted_iota(jnp.int32, (extra, v_ref.shape[2]), 0) == 0).astype(F32).astype(BF16)

    eye_m = eye(model)
    h_ref[tiles - 1, :, :] = jnp.zeros((model, TILE), BF16)
    fetch_x.wait()
    for t in range(tiles):
        size = min(TILE, frames - t * TILE)
        h_ref[t, :, 0:size] = mm_nt(eye_m, x_ref[t * TILE:t * TILE + size, :]).astype(BF16)

    def normalise(z):
        mean = jnp.sum(z, axis=0, keepdims=True) * (1.0 / model)
        c = z - mean
        var = jnp.sum(c * c, axis=0, keepdims=True) * (1.0 / model)
        return c * lax.rsqrt(var + LN_EPSILON)

    for t in range(tiles):
        for lo in range(0, TILE, LANES):
            xhat_ref[t, :, lo:lo + LANES] = normalise(h_ref[t, :, lo:lo + LANES].astype(F32))

    run(plan.step(0, 2))
    run(plan.step(1, 1))
    if layers > 1:
        run(plan.step(2, 1))

    def column(layer, j, lane):
        return wa_ref[layer, j, :, lane:lane + 1].astype(F32)

    def unpack(layer):
        block = 4 * HEAD_DIM
        row = lax.broadcasted_iota(jnp.int32, (block, block), 0)
        col = lax.broadcasted_iota(jnp.int32, (block, block), 1)
        perm = (col == lax.rem(row, HEAD_DIM) * 4 + row // HEAD_DIM).astype(F32).astype(BF16)
        for h in range(heads):
            mixed = mm(perm, g_ref[layer, h * block:(h + 1) * block, 0:aug]).astype(BF16)
            for j in range(4):
                wa_ref[layer, j, h * HEAD_DIM:(h + 1) * HEAD_DIM, :] = mixed[j * HEAD_DIM:(j + 1) * HEAD_DIM]

    scale = HEAD_DIM ** -0.25
    half = TILE // 2
    eye_k = eye(TILE // 2)

    def norm(layer, t, which):
        gain, shift = column(layer, which, model + 1), column(layer, which + 1, model + 1)
        for lo in range(0, TILE, LANES):
            lanes = slice(lo, lo + LANES)
            hat = xhat_ref[t, :, lanes] if (layer, which) == (0, 0) else normalise(h_ref[t, :, lanes].astype(F32))
            a_ref[t, 0:model, lanes] = (hat * gain + shift).astype(BF16)

    def project(layer, t):
        a = a_ref[t]
        kt = (mm(wa_ref[layer, 1], a) * scale).astype(BF16)
        q = (mm(wa_ref[layer, 0], a) * scale).astype(BF16)
        for h in range(heads):
            lo = HEAD_DIM * (h % 2)
            q_ref[h, t, lo:lo + HEAD_DIM, :] = q[h * HEAD_DIM:(h + 1) * HEAD_DIM]
        v = mm(wa_ref[layer, 2], a).astype(BF16)
        for h in range(heads):
            v_ref[h, 0:HEAD_DIM, t * TILE:(t + 1) * TILE] = v[h * HEAD_DIM:(h + 1) * HEAD_DIM]
        for b in range(2):
            kn = mm_nt(eye_k, kt[:, b * half:(b + 1) * half]).astype(BF16)
            for p in range(pairs):
                k_ref[p, t * TILE + b * half:t * TILE + (b + 1) * half, :] = kn[:, p * LANES:(p + 1) * LANES]

    s_refs, m_refs = (s0_ref, s1_ref), (m0_ref, m1_ref)

    blocks = [(lo, min(KEY_BLOCK, keys - lo)) for lo in range(0, keys, KEY_BLOCK)]
    steps = [(hh, t) for hh in range(2) for t in range(tiles)]

    def scores(p, j, c, top):
        (hh, t), (lo, size) = steps[j], blocks[c]
        s_ref = s_refs[j % 2]
        s = mm(k_ref[p, lo:lo + size, :], q_ref[2 * p + hh, t])
        whole = size
        if lo + size > frames:
            whole = size - 8
            row = lax.broadcasted_iota(jnp.int32, (8, TILE), 0) + (lo + whole)
            tail = jnp.where(row < frames, s[whole:], -jnp.inf)
            s_ref[lo + whole:lo + size, :] = tail
            top = jnp.maximum(top, tail)
        s_ref[lo:lo + whole, :] = s[0:whole]
        high = jnp.max(s[0:whole].reshape(whole // 8, 8, TILE), axis=0)
        top = high if top is None else jnp.maximum(top, high)
        if c == len(blocks) - 1:
            m_refs[j % 2][...] = jnp.broadcast_to(jnp.max(top, axis=0, keepdims=True), top.shape)
        return top

    def values(p, j, c, total):
        (hh, t), (lo, size) = steps[j], blocks[c]
        h = 2 * p + hh
        s = s_refs[j % 2][lo:lo + size, :].reshape(size // 8, 8, TILE)
        e = jnp.exp(s - m_refs[j % 2][...][None]).reshape(size, TILE).astype(BF16)
        part = mm(v_ref[h, :, lo:lo + size], e)
        total = part if c == 0 else total + part
        if c == len(blocks) - 1:
            inv = 1.0 / total[HEAD_DIM:HEAD_DIM + 1]
            o_ref[t, pl.ds(pl.multiple_of(h * HEAD_DIM, HEAD_DIM), HEAD_DIM), :] = (total[0:HEAD_DIM] * inv).astype(BF16)
        return total

    def attention(events, before_tail, fillers):
        count = len(blocks)

        def body(p, carry):
            total = acc_ref[...]
            for j in range(len(steps)):
                for at, actions in events.items():
                    if j == 0 and actions:
                        pl.when(p == at)(functools.partial(run, actions))
                top = None
                for c in range(count):
                    top = scores(p, j, c, top)
                    back, at = divmod(j * count + c - LAG - count, count)
                    if back < 0:
                        total = values(jnp.maximum(p - 1, 0), back + len(steps), at, total)
                    else:
                        total = values(p, back, at, total)
            acc_ref[...] = total
            return carry

        lax.fori_loop(0, pairs, body, 0)
        before_tail()
        total = acc_ref[...]
        for k in range(len(steps) * count - LAG - count, len(steps) * count):
            total = values(pairs - 1, *divmod(k, count), total)
            if fillers:
                fillers.pop(0)()

    def unpack_mlp(layer, b):
        w2 = g_ref[layer, b * TILE:(b + 1) * TILE, 2 * aug:2 * aug + model]
        w2t_ref[:, b * TILE:(b + 1) * TILE] = mm_nt(eye_m, w2).astype(BF16)

    def out_project(layer, t):
        r = h_ref[t].astype(F32) + mm(wa_ref[layer, 3], o_ref[t])
        h_ref[t] = r.astype(BF16)

    def mlp(layer, t):
        c = a_ref[t]
        step = 2 * LANES
        for b in range(hidden // step):
            u = mm(g_ref[layer, b * step:(b + 1) * step, aug:2 * aug], c)
            z_ref[b * step:(b + 1) * step, :] = (0.5 * u * (1.0 + lax.erf(u * (2.0 ** -0.5)))).astype(BF16)
        y = h_ref[t].astype(F32) + (mm(w2t_ref[...], z_ref[...]) + column(layer, 0, model + 2))
        h_ref[t] = y.astype(BF16)

    def out_copy(t):
        rows_out = pl.ds(pl.multiple_of(t * TILE, TILE), TILE)
        return pltpu.make_async_copy(y_ref.at[rows_out, :], out_hbm.at[rows_out, :], out_sem.at[t])

    def write_out(t):
        for b in range(2):
            y = mm_nt(eye_k, h_ref[t, :, b * half:(b + 1) * half]).astype(BF16)
            y_ref[pl.ds(pl.multiple_of(t * TILE + b * half, half), half), :] = y
        out_copy(t).start()

    finish(0)
    unpack(0)
    norm(0, 0, 0)
    for t in range(tiles):
        if t + 1 < tiles:
            norm(0, t + 1, 0)
        project(0, t)

    for layer in range(layers):
        more = layer + 1 < layers
        this, after = 2 * layer + 1, 2 * layer + 2
        events = {0: [], 1: [], pairs - 1: []}
        if layer == 0:
            events[0] += plan.step(this, 2)
        elif more:
            events[0] += plan.step(after, 1)
        if more:
            events[1] += plan.step(after, 2) + plan.step(after + 1, 1)
        events[pairs - 1] += plan.hand_over(this, everything=True)
        fillers = [functools.partial(unpack_mlp, layer, b) for b in range(hidden // TILE)]
        fillers.insert(2, functools.partial(out_project, layer, 0))
        fillers += [functools.partial(out_project, layer, 1), functools.partial(norm, layer, 0, 2)]
        attention(events, functools.partial(finish, this), fillers)
        if more:
            run(plan.hand_over(after, everything=True))
        out_project(layer, 2)
        norm(layer, 1, 2)
        mlp(layer, 0)
        if more:
            run(plan.step(after + 1, 2))
            finish(after)
            unpack(layer + 1)
        else:
            write_out(0)
        norm(layer, 2, 2)
        for t in range(1, tiles):
            mlp(layer, t)
            if more:
                norm(layer + 1, t - 1, 0)
            else:
                write_out(t)
        if more:
            for t in range(tiles):
                if t == 1:
                    norm(layer + 1, tiles - 1, 0)
                project(layer + 1, t)

    for piece in range(len(pieces)):
        for m in range(len(MESSAGES)):
            relay(piece, m).wait_send()
        for b in handed(piece):
            hand(piece, b).wait_send()

    for t in range(tiles):
        out_copy(t).wait()


def solution(mesh):
    n = mesh.shape["dp"]

    def body(audio_x, attn_w, fc1_w, fc2_w, vec_d, b1_vec):
        layers, four, model, cols = attn_w.shape
        hidden_cols = fc1_w.shape[2]
        batch, frames, _ = audio_x.shape
        hidden = hidden_cols * n
        aug = model + LANES
        rows = four * cols
        attn = jnp.transpose(attn_w, (0, 3, 1, 2))
        fc1 = jnp.transpose(fc1_w, (0, 2, 1))

        tiles = -(-frames // TILE)
        padded = tiles * TILE
        keys = -(-frames // 16) * 16
        heads = model // HEAD_DIM
        pieces = 2 * layers
        out = pl.pallas_call(
            functools.partial(kernel, n),
            out_shape=jax.ShapeDtypeStruct((padded, model), audio_x.dtype),
            in_specs=[pl.BlockSpec(memory_space=pl.ANY)] * 6,
            out_specs=pl.BlockSpec(memory_space=pl.ANY),
            scratch_shapes=[
                pltpu.VMEM(attn.shape, BF16),
                pltpu.VMEM(fc1.shape, BF16),
                pltpu.VMEM(fc2_w.shape, BF16),
                pltpu.VMEM(vec_d.shape, BF16),
                pltpu.VMEM(b1_vec.shape, BF16),
                pltpu.VMEM((layers, rows, 2 * aug + model), BF16),
                pltpu.VMEM((rows, model), F32),
                pltpu.VMEM((layers, n * rows, 2 * aug + model), BF16),
                pltpu.VMEM((layers, four, model, aug), BF16),
                pltpu.VMEM((model, hidden), BF16),
                pltpu.VMEM((frames, model), BF16),
                pltpu.VMEM((padded, model), BF16),
                pltpu.VMEM((tiles, model, TILE), F32),
                pltpu.VMEM((tiles, model, TILE), BF16),
                pltpu.VMEM((tiles, aug, TILE), BF16),
                pltpu.VMEM((heads, tiles, LANES, TILE), BF16),
                pltpu.VMEM((heads // 2, padded, LANES), BF16),
                pltpu.VMEM((heads, HEAD_DIM + 16, padded), BF16),
                pltpu.VMEM((tiles, aug, TILE), BF16),
                pltpu.VMEM((hidden, TILE), BF16),
                pltpu.VMEM((keys, TILE), F32),
                pltpu.VMEM((keys, TILE), F32),
                pltpu.VMEM((8, TILE), F32),
                pltpu.VMEM((8, TILE), F32),
                pltpu.VMEM((HEAD_DIM + 16, TILE), F32),
                pltpu.SemaphoreType.DMA((6,)),
                pltpu.SemaphoreType.DMA((tiles,)),
                pltpu.SemaphoreType.DMA((pieces, len(MESSAGES))),
                pltpu.SemaphoreType.DMA((pieces, len(MESSAGES))),
                pltpu.SemaphoreType.DMA((pieces, len(BLOCKS) + 1)),
                pltpu.SemaphoreType.DMA((pieces, len(BLOCKS) + 1)),
            ],
            compiler_params=pltpu.CompilerParams(
                collective_id=0, has_side_effects=True, vmem_limit_bytes=60 * 1024 * 1024),
        )(audio_x, attn, fc1, fc2_w, vec_d, b1_vec)
        return out[None, :frames]

    return jax.shard_map(
        body, mesh=mesh,
        in_specs=(P(('rep', 'dp')), P(None, None, None, 'dp'), P(None, None, 'dp'), P(None, 'dp', None), P(None, None, 'dp'), P(None, 'dp')),
        out_specs=P(('rep', 'dp')), check_vma=False)
```
